256 devices in a mesh: samp: 64 (over y, z, core), gene: 4 (over x).
Axes of the slice: x: 4, y: 4, z: 8, core: 2. Of those that a mesh axis runs over, the one named last changes fastest.
Arguments:
- genotypes: int32 [2048, 32768], P('samp', 'gene'), may hold values from -2147483648 to 1789569706, as said below
- allele_freq: float32 [32768], P('gene'), may hold values from 0.035 to 0.56
- sample_weight: float32 [16, 2048], P(None, 'samp'), may hold values from 0.2 to 2
- residual: float32 [16, 2048], P(None, 'samp'), may hold values from -12 to 12
- variant_weight: float32 [32768], P('gene'), may hold values from 0.2 to 4
- block_gene: int32 [256], replicated, may hold values from 0 to 127, as said below
- gene_variants: int32 [128], replicated, may hold values from 1 to 384, as said below
Outputs:
- burden_z: float32 [128], replicated
- skat_z: float32 [128], replicated
The draws below stay inside these ranges and needn't reach their ends.
Inputs may be any that keep to these rules, and one draw needn't show every extreme that they name: Each word holds 16 dosages 0, 1 or 2: bits 2k and 2k+1 of genotypes[i, v] are the dosage of variant slot v in sample (k, i); a dosage 2 in the top field sets the sign bit. `block_gene`: never falling; the blocks come in aligned groups of four, each shared by two consecutive genes, so every gene has 1 to 3 blocks. `gene_variants`: A gene with m blocks has from (m - 1) * 128 + 1 to m * 128 live variants; the slots after them in its last block are padding.
All inputs are finite; a program needn't handle non-finite values.
Results may differ from the reference program's by a relative error of at most 0.0037.
Values sent between devices are 32-bit elements; how exact they have to be, the bound alone decides.
A program may use at most 64 MiB of HBM per device.

```python
import math
import jax
import jax.numpy as jnp
from jax import lax

FIELDS = 16
BLK = 128
ROWS = 2048
SAMPLES = 32768
NBLK = 256
VARIANTS = 32768
NGENE = 128


def gene_layout(key):
    base = jax.random.fold_in(key, 11)
    groups = NBLK // 4
    split_at = jax.random.randint(jax.random.fold_in(base, 1), (groups,), 1, 4, dtype=jnp.int32)
    position = jnp.arange(4, dtype=jnp.int32)
    second = (position[None, :] >= split_at[:, None]).astype(jnp.int32)
    block_gene = (2 * jnp.arange(groups, dtype=jnp.int32)[:, None] + second).reshape(NBLK)
    gene_blocks = jnp.stack([split_at, 4 - split_at], axis=1).reshape(NGENE)
    tail_count = jax.random.randint(jax.random.fold_in(base, 2), (NGENE,), 1, BLK + 1, dtype=jnp.int32)
    return (block_gene, (gene_blocks - 1) * BLK + tail_count)


def draw_block_gene(key, part):
    return gene_layout(key)[0]


def draw_gene_variants(key, part):
    return gene_layout(key)[1]


def allele_levels(key):
    base = jax.random.fold_in(jax.random.fold_in(key, 21), 5)
    return jax.random.randint(base, (VARIANTS,), 40, 520, dtype=jnp.int32)


def draw_allele_freq(key, part):
    levels = allele_levels(key).astype(jnp.float32) / 1024.0
    return levels


def draw_genotypes(key, part):
    levels = allele_levels(key)
    base = jax.random.fold_in(key, 21)
    column = jnp.arange(VARIANTS, dtype=jnp.int32)

    def one_field(field_index, packed):
        field_key = jax.random.fold_in(base, field_index + 100)
        dosage = jnp.zeros((ROWS, VARIANTS), jnp.int32)
        for strand in range(2):
            strand_key = jax.random.fold_in(field_key, strand)
            fresh_bits = (jax.random.randint(jax.random.fold_in(strand_key, 1), (ROWS, VARIANTS), 0, 1024, dtype=jnp.int32) < levels[None, :]).astype(jnp.int32)
            restart = jax.random.randint(jax.random.fold_in(strand_key, 2), (ROWS, VARIANTS), 0, 5, dtype=jnp.int32) == 0
            restart = jnp.logical_or(restart, column[None, :] == 0)
            source = lax.cummax(jnp.where(restart, column[None, :], 0), axis=1)
            dosage = dosage + jnp.take_along_axis(fresh_bits, source, axis=1)
        return packed + jnp.left_shift(dosage, 2 * field_index)
    return lax.fori_loop(0, FIELDS, one_field, jnp.zeros((ROWS, VARIANTS), jnp.int32))


def draw_residual(key, part):
    row_index = jnp.arange(ROWS, dtype=jnp.float32)
    spread = 1.0 + row_index / ROWS
    values = jax.random.truncated_normal(key, -6.0, 6.0, (FIELDS, ROWS), jnp.float32)
    return values * spread[None, :]


def shard_levels(key, extent, shards, low, largest):
    gain, own = 1.0, jax.random.fold_in(key, 6)
    for dim, shards_of in shards:
        draws = jnp.exp(jax.random.uniform(jax.random.fold_in(own, dim), (shards_of,), jnp.float32, low / len(shards), largest / len(shards)))
        gain = gain * jnp.repeat(draws, extent[dim] // shards_of).reshape([-1 if axis == dim else 1 for axis in range(len(extent))])
    return gain


def setup_inputs(seed: int = 0) -> dict:
    streams_of = jax.random.split(jax.random.key(seed), 8)
    return {
        "genotypes": draw_genotypes(jax.random.fold_in(streams_of[7], 71), 0),
        "allele_freq": draw_allele_freq(jax.random.fold_in(streams_of[7], 71), 0),
        "sample_weight": jnp.clip(jnp.exp(math.log(2.0) - 2.3025851 * jax.random.uniform(streams_of[2], (FIELDS, ROWS), jnp.float32) ** shard_levels(streams_of[2], (FIELDS, ROWS), ((1, 64),), -0.2, 0.2)), 0.2, 2.0),
        "residual": draw_residual(jax.random.fold_in(streams_of[7], 71), 0),
        "variant_weight": jnp.clip(jnp.exp(math.log(4.0) - 2.9957323 * jax.random.uniform(streams_of[4], (VARIANTS,), jnp.float32) ** shard_levels(streams_of[4], (VARIANTS,), ((0, 4),), -0.2, 0.2)), 0.2, 4.0),
        "block_gene": draw_block_gene(jax.random.fold_in(streams_of[7], 71), 0),
        "gene_variants": draw_gene_variants(jax.random.fold_in(streams_of[7], 71), 0),
    }


def unpack(packed_words, allele_part, root_weight):
    offsets = 2 * jnp.arange(FIELDS, dtype=jnp.int32)
    dosage = jnp.bitwise_and(jnp.right_shift(packed_words[None, :, :], offsets[:, None, None]), 3)
    centered = dosage.astype(jnp.float32) - 2.0 * allele_part[None, None, :]
    return (root_weight[:, :, None] * centered).astype(jnp.bfloat16)

def block_stats(gram_part, scores, effective):
    weighted_score = effective * scores
    burden_sum = lax.optimization_barrier(jnp.sum(weighted_score, axis=1))
    skat_sum = lax.optimization_barrier(jnp.sum(weighted_score * weighted_score, axis=1))
    image = jnp.einsum('buv,bv->bu', gram_part, effective, precision=lax.Precision.HIGHEST)
    burden_var = lax.optimization_barrier(jnp.sum(effective * image, axis=1))
    diagonal = jnp.diagonal(gram_part, axis1=1, axis2=2)
    trace_one = lax.optimization_barrier(jnp.sum(effective * effective * diagonal, axis=1))
    scaled_gram = effective[:, :, None] * gram_part * effective[:, None, :]
    trace_two = lax.optimization_barrier(jnp.sum(scaled_gram * scaled_gram, axis=(1, 2)))
    return jnp.stack([burden_sum, burden_var, skat_sum, trace_one, trace_two])

def reference(genotypes, allele_freq, sample_weight, residual, variant_weight, block_gene, gene_variants):
    root_weight = jnp.sqrt(sample_weight)
    weighted_residual = (root_weight * residual).astype(jnp.bfloat16).reshape(1, FIELDS * ROWS)
    widened_residual = weighted_residual.astype(jnp.float32)
    variance = jnp.sum(sample_weight * residual * residual) / SAMPLES

    def block_terms(block_index):
        packed_words = lax.dynamic_slice_in_dim(genotypes, block_index * BLK, BLK, 1)
        allele_part = lax.dynamic_slice_in_dim(allele_freq, block_index * BLK, BLK, 0)
        scaled = unpack(packed_words, allele_part, root_weight).reshape(FIELDS * ROWS, BLK)
        widened = scaled.astype(jnp.float32)
        gram_part = jnp.dot(widened.T, widened, precision=lax.Precision.HIGHEST)
        score = jnp.dot(widened_residual, widened, precision=lax.Precision.HIGHEST)[0]
        return (gram_part, score)
    block_index = jnp.arange(NBLK, dtype=jnp.int32)
    gram_all, score_all = lax.map(block_terms, block_index)
    first_block = lax.optimization_barrier(jnp.sum((block_gene[None, :] < block_gene[:, None]).astype(jnp.int32), axis=1))
    counted = gene_variants[block_gene]
    column = jnp.arange(BLK, dtype=jnp.int32)
    is_live = (block_index - first_block)[:, None] * BLK + column[None, :] < counted[:, None]
    effective = variant_weight.reshape(NBLK, BLK) * is_live.astype(jnp.float32)
    stats = block_stats(gram_all, score_all, effective)
    member = (block_gene[:, None] == jnp.arange(NGENE, dtype=jnp.int32)[None, :]).astype(jnp.float32)
    totals = jnp.dot(stats, member, precision=lax.Precision.HIGHEST)
    burden_z = totals[0] / jnp.sqrt(variance * totals[1])
    skat_z = (totals[2] - variance * totals[3]) / (variance * jnp.sqrt(2.0 * totals[4]))
    return (burden_z, skat_z)
```

```python
import functools

import jax
import jax.numpy as jnp
from jax import lax
from jax.experimental import pallas as pl
from jax.experimental.pallas import tpu as pltpu
from jax.sharding import Mesh
from jax.sharding import PartitionSpec as P

BLK = 128
FIELDS = 16
MESH = pl.DeviceIdType.MESH
F32 = jnp.float32
BF16 = jnp.bfloat16
TAIL = 8


def total(x):
    return jnp.sum(jnp.sum(x, axis=1, keepdims=True), axis=0, keepdims=True)


def masked(words, k):
    if k == FIELDS - 1:
        words, k = jnp.right_shift(words, 2), k - 1
    return jnp.bitwise_and(words, 3 << (2 * k)).astype(F32)


def kernel(
    sizes, genotypes, freq, weight, residual, variant_weight, block_gene, gene_variants, out,
    staged, words, weights_in, residuals_in, rhs, lhs, scale, tail, part, gathered, freq_v, vw_v, bg_v, gv_v,
    rows_one, rows_two, out_v, stage_sem, small_sem, word_recv, word_send, side_recv, side_send,
    part_recv, part_send, one_recv, one_send, two_recv, two_send, out_sem,
):
    ny, nz, nc, nx = sizes
    rows = genotypes.shape[0]
    depth = ny * nc * rows
    genes_here = nz * nc // 2
    y, z, c, x = (lax.axis_index(a) for a in ("y", "z", "c", "x"))
    mine = y * nc + c

    stage = pltpu.make_async_copy(genotypes, staged, stage_sem)
    stage.start()
    smalls = [
        pltpu.make_async_copy(src, dst, small_sem.at[i])
        for i, (src, dst) in enumerate(
            ((freq, freq_v), (variant_weight, vw_v), (block_gene, bg_v), (gene_variants, gv_v))
        )
    ]
    for copy in smalls:
        copy.start()

    def near(dy, dc):
        return (lax.rem(y + dy, ny), z, lax.rem(c + dc, nc), x)

    def along(dz, dc):
        return (y, lax.rem(z + dz, nz), lax.rem(c + dc, nc), x)

    def across(dx, dy):
        return (lax.rem(y + dy, ny), z, c, lax.rem(x + dx, nx))

    order = sorted(range(1, ny), key=lambda d: -min(d, ny - d))
    near_peers = [(dy, dc) for dy in order + [0] for dc in range(nc) if (dy, dc) != (0, 0)]
    along_peers = [(dz, dc) for dz in range(nz) for dc in range(nc) if (dz, dc) != (0, 0)]
    across_peers = [(dx, dy) for dx in range(nx) for dy in range(ny) if (dx, dy) != (0, 0)]
    greeted = [near(*p) for p in near_peers]
    greeted += [along(*p) for p in along_peers if p[0] != 0]
    greeted += [across(*p) for p in across_peers if p[0] != 0]
    barrier = pltpu.get_barrier_semaphore()
    for peer in greeted:
        pl.semaphore_signal(barrier, inc=1, device_id=peer, device_id_type=MESH)
    pl.semaphore_wait(barrier, len(greeted))

    own_side = []
    for i, (src, dst) in enumerate(((weight, weights_in), (residual, residuals_in))):
        for peer in near_peers:
            pltpu.make_async_remote_copy(
                src_ref=src, dst_ref=dst.at[mine], send_sem=side_send.at[i], recv_sem=side_recv.at[i],
                device_id=near(*peer), device_id_type=MESH,
            ).start()
        copy = pltpu.make_async_copy(src, dst.at[mine], side_recv.at[i])
        copy.start()
        own_side.append(copy)

    def owner_of(j):
        distance = nz // 2 - (j + 1) // 2
        sign = 2 * (j % 2) - 1
        return lax.rem(z + sign * distance + nz, nz)

    stage.wait()

    def send_words(j, carry):
        zo = owner_of(j)
        for dy, dc in near_peers:
            to = near(dy, dc)
            column = pl.multiple_of(((to[0] * nz + zo) * nc + to[2]) * BLK, BLK)
            pltpu.make_async_remote_copy(
                src_ref=staged.at[:, pl.ds(column, BLK)], dst_ref=words.at[j, mine],
                send_sem=word_send, recv_sem=word_recv.at[j],
                device_id=to, device_id_type=MESH,
            ).start()
        column = pl.multiple_of(((y * nz + zo) * nc + c) * BLK, BLK)
        pltpu.make_async_copy(
            genotypes.at[:, pl.ds(column, BLK)], words.at[j, mine], word_recv.at[j]
        ).start()
        return carry

    lax.fori_loop(0, nz, send_words, 0)

    for i, dst in enumerate((weights_in, residuals_in)):
        pltpu.make_async_copy(dst, dst, side_recv.at[i]).wait()
    weight_all = jnp.concatenate([weights_in[g] for g in range(ny * nc)], axis=1)
    residual_all = jnp.concatenate([residuals_in[g] for g in range(ny * nc)], axis=1)
    rounded = weight_all.astype(BF16).astype(F32)
    cross = weight_all * residual_all
    high = cross.astype(BF16).astype(F32)
    low = (cross - high).astype(BF16).astype(F32)
    field = lax.broadcasted_iota(jnp.int32, (FIELDS, 1), 0)
    inverse = jnp.ones((FIELDS, 1), F32)
    for k in range(1, FIELDS):
        inverse = jnp.where(field == k, 0.25 ** min(k, FIELDS - 2), inverse)
    scale[...] = rounded * (inverse * inverse)
    extra = [a * inverse for a in (rounded, high, low)]
    row_id = lax.broadcasted_iota(jnp.int32, (2 * TAIL, depth), 0)
    for k in range(FIELDS):
        rows_k = jnp.zeros((2 * TAIL, depth), F32)
        for i, a in enumerate(extra):
            rows_k = jnp.where(row_id == i, a[k : k + 1], rows_k)
        lhs[BLK : BLK + 2 * TAIL, k * depth : (k + 1) * depth] = rows_k.astype(BF16)
    sums = (total(rounded), total(high + low), total(cross * residual_all))
    lane = lax.broadcasted_iota(jnp.int32, (TAIL, BLK), 1)
    sublane = lax.broadcasted_iota(jnp.int32, (TAIL, BLK), 0)
    tail_rows = jnp.zeros((TAIL, BLK), F32)
    for i, s in enumerate(sums):
        tail_rows = jnp.where(sublane == 3 + i, s, tail_rows)
    tail[...] = tail_rows

    def partial(j):
        pltpu.make_async_copy(words.at[j], words.at[j], word_recv.at[j]).wait()
        block = words[j].reshape(depth, BLK)
        turned = jnp.transpose(block)
        for k in range(FIELDS):
            rhs[k * depth : (k + 1) * depth, :] = masked(block, k).astype(BF16)
            lhs[:BLK, k * depth : (k + 1) * depth] = (masked(turned, k) * scale[k : k + 1, :]).astype(BF16)
        gram = jnp.dot(lhs[...], rhs[...], preferred_element_type=F32)
        part[j, :BLK] = gram[:BLK]
        part[j, BLK:] = gram[BLK : BLK + TAIL] + tail[...]

    def far_block(j, carry):
        partial(j)
        pltpu.make_async_remote_copy(
            src_ref=part.at[j], dst_ref=gathered.at[j], send_sem=part_send, recv_sem=part_recv,
            device_id=(y, owner_of(j), c, x), device_id_type=MESH,
        ).start()
        return carry

    lax.fori_loop(0, nz - 1, far_block, 0)
    partial(nz - 1)

    for copy in smalls:
        copy.wait()
    own = (y * nz + z) * nc + c
    doubled = 2.0 * freq_v[pl.ds(own, 1), :]
    own_block = x * (ny * nz * nc) + own
    bg = bg_v[...]
    block_id = lax.broadcasted_iota(jnp.int32, bg.shape, 0) * BLK + lax.broadcasted_iota(jnp.int32, bg.shape, 1)
    gene = total(jnp.where(block_id == own_block, bg, 0))
    first = total((bg < gene).astype(jnp.int32))
    row_lane = lax.broadcasted_iota(jnp.int32, (1, BLK), 1)
    counted = total(jnp.where(row_lane == gene, gv_v[...], 0))
    live = (own_block - first) * BLK + row_lane < counted
    effective = jnp.where(live, vw_v[pl.ds(own, 1), :], 0.0)

    pltpu.make_async_copy(gathered, gathered, part_recv).wait()
    summed = part[nz - 1]
    for j in range(nz - 1):
        summed = summed + gathered[j]
    raw = summed[:BLK]
    linear = summed[BLK : BLK + 1]
    weight_sum = summed[BLK + 3 : BLK + 4]
    score = summed[BLK + 1 : BLK + 2] + summed[BLK + 2 : BLK + 3] - doubled * summed[BLK + 4 : BLK + 5]
    down = lax.broadcasted_iota(jnp.int32, (BLK, BLK), 0)
    side = lax.broadcasted_iota(jnp.int32, (BLK, BLK), 1)
    stacked = jnp.where(down == 0, doubled, jnp.where(down == 1, linear, jnp.where(down == 2, effective, 0.0)))
    upright = jnp.transpose(stacked)
    doubled_c, linear_c, effective_c = upright[:, 0:1], upright[:, 1:2], upright[:, 2:3]
    gram = raw - doubled_c * (linear - doubled * weight_sum) - linear_c * doubled
    scaled = effective_c * gram * effective
    weighted_score = effective * score
    stats = (
        total(weighted_score),
        total(scaled),
        total(weighted_score * weighted_score),
        total(jnp.where(down == side, scaled, 0.0)),
        total(scaled * scaled),
    )
    near_gene = gene - (x * ny + y) * genes_here
    row = jnp.zeros((1, BLK), F32)
    for i, s in enumerate(stats):
        row = jnp.where(row_lane == i * genes_here + near_gene, s, row)
    at_variance = len(stats) * genes_here
    share = jnp.where(c == 0, tail[5:6, :], 0.0)
    row = jnp.where(row_lane == at_variance, share, row)
    seat = z * nc + c
    rows_one[seat] = row
    for peer in along_peers:
        pltpu.make_async_remote_copy(
            src_ref=rows_one.at[seat], dst_ref=rows_one.at[seat], send_sem=one_send, recv_sem=one_recv,
            device_id=along(*peer), device_id_type=MESH,
        ).start()
    count = nz * nc - 1
    pltpu.make_async_copy(rows_one.at[pl.ds(0, count)], rows_one.at[pl.ds(0, count)], one_recv).wait()
    genes = rows_one[0]
    for i in range(1, count + 1):
        genes = genes + rows_one[i]

    place = x * ny + y
    samples = depth * nz * FIELDS
    variance = total(jnp.where(row_lane == at_variance, genes, 0.0)) / samples
    totals = [
        pltpu.roll(genes, lax.rem(place * genes_here - i * genes_here + BLK, BLK), 1)
        for i in range(len(stats))
    ]
    here = jnp.logical_and(row_lane >= place * genes_here, row_lane < (place + 1) * genes_here)
    totals = [jnp.where(here, t, 1.0) for t in totals]
    burden = totals[0] / jnp.sqrt(variance * totals[1])
    skat = (totals[2] - variance * totals[3]) / (variance * jnp.sqrt(2.0 * totals[4]))
    pair_row = lax.broadcasted_iota(jnp.int32, (2, BLK), 0)
    rows_two[place] = jnp.where(here, jnp.where(pair_row == 0, burden, skat), 0.0)
    for peer in across_peers:
        pltpu.make_async_remote_copy(
            src_ref=rows_two.at[place], dst_ref=rows_two.at[place], send_sem=two_send, recv_sem=two_recv,
            device_id=across(*peer), device_id_type=MESH,
        ).start()
    count = nx * ny - 1
    pltpu.make_async_copy(rows_two.at[pl.ds(0, count)], rows_two.at[pl.ds(0, count)], two_recv).wait()
    scores = rows_two[0]
    for i in range(1, count + 1):
        scores = scores + rows_two[i]
    out[...] = scores

    sent = len(near_peers)
    for i, dst in enumerate((weights_in, residuals_in)):
        pltpu.make_async_copy(dst.at[pl.ds(0, sent)], dst.at[pl.ds(0, sent)], side_send.at[i]).wait()
    span = words.at[:, pl.ds(0, sent)]
    pltpu.make_async_copy(span, span, word_send).wait()
    pltpu.make_async_copy(gathered, gathered, part_send).wait()
    span = rows_one.at[pl.ds(0, len(along_peers))]
    pltpu.make_async_copy(span, span, one_send).wait()
    span = rows_two.at[pl.ds(0, len(across_peers))]
    pltpu.make_async_copy(span, span, two_send).wait()


def local(
    sizes, genotypes, allele_freq, sample_weight, residual, variant_weight, block_gene, gene_variants
):
    ny, nz, nc, nx = sizes
    rows, columns = genotypes.shape
    group = ny * nc
    depth = group * rows
    blocks = columns // BLK
    args = (
        genotypes,
        allele_freq.reshape(blocks, BLK),
        sample_weight,
        residual,
        variant_weight.reshape(blocks, BLK),
        block_gene.reshape(-1, BLK),
        gene_variants.reshape(1, -1),
    )
    anywhere = pl.BlockSpec(memory_space=pl.ANY)
    dma = pltpu.SemaphoreType.DMA
    scores = pl.pallas_call(
        functools.partial(kernel, sizes),
        out_shape=jax.ShapeDtypeStruct((2, BLK), F32),
        in_specs=[anywhere] * len(args),
        out_specs=pl.BlockSpec(memory_space=pltpu.VMEM),
        scratch_shapes=[
            pltpu.VMEM((rows, columns), jnp.int32),
            pltpu.VMEM((nz, group, rows, BLK), jnp.int32),
            pltpu.VMEM((group, FIELDS, rows), F32),
            pltpu.VMEM((group, FIELDS, rows), F32),
            pltpu.VMEM((FIELDS * depth, BLK), BF16),
            pltpu.VMEM((BLK + 2 * TAIL, FIELDS * depth), BF16),
            pltpu.VMEM((FIELDS, depth), F32),
            pltpu.VMEM((TAIL, BLK), F32),
            pltpu.VMEM((nz, BLK + TAIL, BLK), F32),
            pltpu.VMEM((nz - 1, BLK + TAIL, BLK), F32),
            pltpu.VMEM(args[1].shape, F32),
            pltpu.VMEM(args[4].shape, F32),
            pltpu.VMEM(args[5].shape, jnp.int32),
            pltpu.VMEM(args[6].shape, jnp.int32),
            pltpu.VMEM((nz * nc, 1, BLK), F32),
            pltpu.VMEM((nx * ny, 2, BLK), F32),
            pltpu.VMEM((2, BLK), F32),
            dma, dma((4,)), dma((nz,)), dma, dma((2,)), dma((2,)),
            dma, dma, dma, dma, dma, dma, dma,
        ],
        compiler_params=pltpu.CompilerParams(collective_id=0, has_side_effects=True),
    )(*args)
    return (scores[0], scores[1])


def solution(mesh):
    nx = mesh.shape["gene"]
    sizes = (4, 8, 2, nx)
    torus = Mesh(mesh.devices.reshape(sizes), ("y", "z", "c", "x"))
    samp = ("y", "z", "c")
    placed = (P(samp, "x"), P("x"), P(None, samp), P(None, samp), P("x"), P(), P())
    step = functools.partial(local, sizes)
    return jax.shard_map(step, mesh=torus, in_specs=placed, out_specs=(P(), P()), check_vma=False)
```

```python
import functools

import jax
import jax.numpy as jnp
from jax import lax
from jax.experimental import pallas as pl
from jax.experimental.pallas import tpu as pltpu
from jax.sharding import Mesh
from jax.sharding import PartitionSpec as P

BLK = 128
HALF = BLK // 2
FIELDS = 16
MESH = pl.DeviceIdType.MESH
F32 = jnp.float32
BF16 = jnp.bfloat16
TAIL = 8


def total(x):
    return jnp.sum(jnp.sum(x, axis=1, keepdims=True), axis=0, keepdims=True)


def masked(words, k):
    if k == FIELDS - 1:
        words, k = jnp.right_shift(words, 2), k - 1
    return jnp.bitwise_and(words, 3 << (2 * k)).astype(F32)


def kernel(
    sizes, genotypes, freq, weight, residual, variant_weight, block_gene, gene_variants, out,
    staged, words, weights_in, residuals_in, rhs, lhs, scale, tail, part, gathered, freq_v, vw_v, bg_v, gv_v,
    rows_one, rows_two, stage_sem, small_sem, word_recv, word_send, side_recv, side_send,
    part_recv, part_send, one_recv, one_send, two_recv, two_send,
):
    ny, nz, nc, nx = sizes
    rows = genotypes.shape[0]
    depth = ny * nc * rows
    genes_here = nz * nc // 2
    y, z, c, x = (lax.axis_index(a) for a in ("y", "z", "c", "x"))
    mine = y * nc + c

    stage = pltpu.make_async_copy(genotypes, staged, stage_sem)
    stage.start()
    smalls = [
        pltpu.make_async_copy(src, dst, small_sem.at[i])
        for i, (src, dst) in enumerate(
            ((freq, freq_v), (variant_weight, vw_v), (block_gene, bg_v), (gene_variants, gv_v))
        )
    ]
    for copy in smalls:
        copy.start()

    def near(dy, dc):
        return (lax.rem(y + dy, ny), z, lax.rem(c + dc, nc), x)

    def along(dz, dc):
        return (y, lax.rem(z + dz, nz), lax.rem(c + dc, nc), x)

    def across(dx, dy):
        return (lax.rem(y + dy, ny), z, c, lax.rem(x + dx, nx))

    order = sorted(range(1, ny), key=lambda d: -min(d, ny - d))
    near_peers = [(dy, dc) for dy in order + [0] for dc in range(nc) if (dy, dc) != (0, 0)]
    along_peers = [(dz, dc) for dz in range(nz) for dc in range(nc) if (dz, dc) != (0, 0)]
    across_peers = [(dx, dy) for dx in range(nx) for dy in range(ny) if (dx, dy) != (0, 0)]
    greeted = [near(*p) for p in near_peers]
    greeted += [along(*p) for p in along_peers if p[0] != 0]
    greeted += [across(*p) for p in across_peers if p[0] != 0]
    barrier = pltpu.get_barrier_semaphore()
    for peer in greeted:
        pl.semaphore_signal(barrier, inc=1, device_id=peer, device_id_type=MESH)
    pl.semaphore_wait(barrier, len(greeted))

    own_side = []
    for i, (src, dst) in enumerate(((weight, weights_in), (residual, residuals_in))):
        for peer in near_peers:
            pltpu.make_async_remote_copy(
                src_ref=src, dst_ref=dst.at[mine], send_sem=side_send.at[i], recv_sem=side_recv.at[i],
                device_id=near(*peer), device_id_type=MESH,
            ).start()
        copy = pltpu.make_async_copy(src, dst.at[mine], side_recv.at[i])
        copy.start()
        own_side.append(copy)

    def owner_of(j):
        distance = nz // 2 - (j + 1) // 2
        sign = 2 * (j % 2) - 1
        return lax.rem(z + sign * distance + nz, nz)

    stage.wait()

    def send_words(j, carry):
        zo = owner_of(j)
        for dy, dc in near_peers:
            to = near(dy, dc)
            column = pl.multiple_of(((to[0] * nz + zo) * nc + to[2]) * BLK, BLK)
            pltpu.make_async_remote_copy(
                src_ref=staged.at[:, pl.ds(column, BLK)], dst_ref=words.at[j, mine],
                send_sem=word_send, recv_sem=word_recv.at[j],
                device_id=to, device_id_type=MESH,
            ).start()
        column = pl.multiple_of(((y * nz + zo) * nc + c) * BLK, BLK)
        pltpu.make_async_copy(
            genotypes.at[:, pl.ds(column, BLK)], words.at[j, mine], word_recv.at[j]
        ).start()
        return carry

    lax.fori_loop(0, nz, send_words, 0)

    for i, dst in enumerate((weights_in, residuals_in)):
        pltpu.make_async_copy(dst, dst, side_recv.at[i]).wait()
    weight_all = jnp.concatenate([weights_in[g] for g in range(ny * nc)], axis=1)
    residual_all = jnp.concatenate([residuals_in[g] for g in range(ny * nc)], axis=1)
    rounded = weight_all.astype(BF16).astype(F32)
    cross = weight_all * residual_all
    high = cross.astype(BF16).astype(F32)
    low = (cross - high).astype(BF16).astype(F32)
    field = lax.broadcasted_iota(jnp.int32, (FIELDS, 1), 0)
    inverse = jnp.ones((FIELDS, 1), F32)
    for k in range(1, FIELDS):
        inverse = jnp.where(field == k, 0.25 ** min(k, FIELDS - 2), inverse)
    scale[...] = rounded * (inverse * inverse)
    extra = [a * inverse for a in (rounded, high, low)]
    row_id = lax.broadcasted_iota(jnp.int32, (2 * TAIL, depth), 0)
    for k in range(FIELDS):
        rows_k = jnp.zeros((2 * TAIL, depth), F32)
        for i, a in enumerate(extra):
            rows_k = jnp.where(row_id == i, a[k : k + 1], rows_k)
        lhs[BLK : BLK + 2 * TAIL, k * depth : (k + 1) * depth] = rows_k.astype(BF16)
    sums = (total(rounded), total(high + low), total(cross * residual_all))
    lane = lax.broadcasted_iota(jnp.int32, (TAIL, BLK), 1)
    sublane = lax.broadcasted_iota(jnp.int32, (TAIL, BLK), 0)
    tail_rows = jnp.zeros((TAIL, BLK), F32)
    for i, s in enumerate(sums):
        tail_rows = jnp.where(sublane == 3 + i, s, tail_rows)
    tail[...] = tail_rows
    fold_down = lax.broadcasted_iota(jnp.int32, (HALF, BLK), 0)
    fold_side = lax.broadcasted_iota(jnp.int32, (HALF, BLK), 1)
    folded = jnp.logical_and(fold_side >= HALF, fold_down >= fold_side - HALF)

    def partial(j):
        pltpu.make_async_copy(words.at[j], words.at[j], word_recv.at[j]).wait()
        block = words[j].reshape(depth, BLK)
        turned = jnp.transpose(block)
        for k in range(FIELDS):
            rhs[k * depth : (k + 1) * depth, :] = masked(block, k).astype(BF16)
            lhs[:BLK, k * depth : (k + 1) * depth] = (masked(turned, k) * scale[k : k + 1, :]).astype(BF16)
        gram = jnp.dot(lhs[...], rhs[...], preferred_element_type=F32)
        low_rows = gram[HALF:BLK]
        part[j, :HALF] = jnp.where(folded, pltpu.roll(gram[:HALF], HALF, 1), low_rows)
        corner = jnp.sum(jnp.where(fold_side - HALF == fold_down, low_rows, 0.0), axis=0, keepdims=True)
        part[j, HALF:] = gram[BLK : BLK + TAIL] + jnp.where(sublane == 6, corner, tail[...])

    def far_block(j, carry):
        partial(j)
        pltpu.make_async_remote_copy(
            src_ref=part.at[j], dst_ref=gathered.at[j], send_sem=part_send, recv_sem=part_recv,
            device_id=(y, owner_of(j), c, x), device_id_type=MESH,
        ).start()
        return carry

    lax.fori_loop(0, nz - 1, far_block, 0)
    partial(nz - 1)

    for copy in smalls:
        copy.wait()
    own = (y * nz + z) * nc + c
    doubled = 2.0 * freq_v[pl.ds(own, 1), :]
    own_block = x * (ny * nz * nc) + own
    bg = bg_v[...]
    block_id = lax.broadcasted_iota(jnp.int32, bg.shape, 0) * BLK + lax.broadcasted_iota(jnp.int32, bg.shape, 1)
    gene = total(jnp.where(block_id == own_block, bg, 0))
    first = total((bg < gene).astype(jnp.int32))
    row_lane = lax.broadcasted_iota(jnp.int32, (1, BLK), 1)
    counted = total(jnp.where(row_lane == gene, gv_v[...], 0))
    live = (own_block - first) * BLK + row_lane < counted
    effective = jnp.where(live, vw_v[pl.ds(own, 1), :], 0.0)

    pltpu.make_async_copy(gathered, gathered, part_recv).wait()
    summed = part[nz - 1]
    for j in range(nz - 1):
        summed = summed + gathered[j]
    ends = summed[HALF:]
    linear, weight_sum = ends[0:1], ends[3:4]
    score = ends[1:2] + ends[2:3] - doubled * ends[4:5]
    down = lax.broadcasted_iota(jnp.int32, (BLK, BLK), 0)
    stacked = jnp.where(down == 0, doubled, jnp.where(down == 1, linear, jnp.where(down == 2, effective, 0.0)))
    upright = jnp.transpose(stacked)

    def by_row(i):
        return jnp.where(folded, upright[:HALF, i : i + 1], upright[HALF:, i : i + 1])

    def by_lane(row):
        return jnp.where(folded, pltpu.roll(row, HALF, 1), row)

    doubled_v, linear_v = by_lane(doubled), by_lane(linear)
    gram = summed[:HALF] - by_row(0) * (linear_v - doubled_v * weight_sum) - by_row(1) * doubled_v
    scaled = by_row(2) * gram * by_lane(effective)
    first_diagonal = fold_side - HALF == fold_down
    twice = jnp.where(first_diagonal, 1.0, 2.0) * scaled
    corner = ends[6:7] - doubled * (2.0 * linear - doubled * weight_sum)
    corner = jnp.where(row_lane >= HALF, effective * effective * corner, 0.0)
    weighted_score = effective * score
    stats = (
        total(weighted_score),
        total(twice) + total(corner),
        total(weighted_score * weighted_score),
        total(jnp.where(first_diagonal, scaled, 0.0)) + total(corner),
        total(twice * scaled) + total(corner * corner),
    )
    near_gene = gene - (x * ny + y) * genes_here
    row = jnp.zeros((1, BLK), F32)
    for i, s in enumerate(stats):
        row = jnp.where(row_lane == i * genes_here + near_gene, s, row)
    at_variance = len(stats) * genes_here
    share = jnp.where(c == 0, tail[5:6, :], 0.0)
    row = jnp.where(row_lane == at_variance, share, row)
    seat = z * nc + c
    rows_one[seat] = row
    for peer in along_peers:
        pltpu.make_async_remote_copy(
            src_ref=rows_one.at[seat], dst_ref=rows_one.at[seat], send_sem=one_send, recv_sem=one_recv,
            device_id=along(*peer), device_id_type=MESH,
        ).start()
    count = nz * nc - 1
    pltpu.make_async_copy(rows_one.at[pl.ds(0, count)], rows_one.at[pl.ds(0, count)], one_recv).wait()
    genes = rows_one[0]
    for i in range(1, count + 1):
        genes = genes + rows_one[i]

    place = x * ny + y
    samples = depth * nz * FIELDS
    variance = total(jnp.where(row_lane == at_variance, genes, 0.0)) / samples
    totals = [
        pltpu.roll(genes, lax.rem(place * genes_here - i * genes_here + BLK, BLK), 1)
        for i in range(len(stats))
    ]
    here = jnp.logical_and(row_lane >= place * genes_here, row_lane < (place + 1) * genes_here)
    totals = [jnp.where(here, t, 1.0) for t in totals]
    burden = totals[0] / jnp.sqrt(variance * totals[1])
    skat = (totals[2] - variance * totals[3]) / (variance * jnp.sqrt(2.0 * totals[4]))
    pair_row = lax.broadcasted_iota(jnp.int32, (2, BLK), 0)
    rows_two[place] = jnp.where(here, jnp.where(pair_row == 0, burden, skat), 0.0)
    for peer in across_peers:
        pltpu.make_async_remote_copy(
            src_ref=rows_two.at[place], dst_ref=rows_two.at[place], send_sem=two_send, recv_sem=two_recv,
            device_id=across(*peer), device_id_type=MESH,
        ).start()
    count = nx * ny - 1
    pltpu.make_async_copy(rows_two.at[pl.ds(0, count)], rows_two.at[pl.ds(0, count)], two_recv).wait()
    scores = rows_two[0]
    for i in range(1, count + 1):
        scores = scores + rows_two[i]
    out[...] = scores

    sent = len(near_peers)
    for i, dst in enumerate((weights_in, residuals_in)):
        pltpu.make_async_copy(dst.at[pl.ds(0, sent)], dst.at[pl.ds(0, sent)], side_send.at[i]).wait()
    span = words.at[:, pl.ds(0, sent)]
    pltpu.make_async_copy(span, span, word_send).wait()
    pltpu.make_async_copy(gathered, gathered, part_send).wait()
    span = rows_one.at[pl.ds(0, len(along_peers))]
    pltpu.make_async_copy(span, span, one_send).wait()
    span = rows_two.at[pl.ds(0, len(across_peers))]
    pltpu.make_async_copy(span, span, two_send).wait()


def local(
    sizes, genotypes, allele_freq, sample_weight, residual, variant_weight, block_gene, gene_variants
):
    ny, nz, nc, nx = sizes
    rows, columns = genotypes.shape
    group = ny * nc
    depth = group * rows
    blocks = columns // BLK
    args = (
        genotypes,
        allele_freq.reshape(blocks, BLK),
        sample_weight,
        residual,
        variant_weight.reshape(blocks, BLK),
        block_gene.reshape(-1, BLK),
        gene_variants.reshape(1, -1),
    )
    anywhere = pl.BlockSpec(memory_space=pl.ANY)
    dma = pltpu.SemaphoreType.DMA
    scores = pl.pallas_call(
        functools.partial(kernel, sizes),
        out_shape=pltpu.VMEM((2, BLK), F32),
        in_specs=[anywhere] * len(args),
        out_specs=pl.BlockSpec(memory_space=pltpu.VMEM),
        scratch_shapes=[
            pltpu.VMEM((rows, columns), jnp.int32),
            pltpu.VMEM((nz, group, rows, BLK), jnp.int32),
            pltpu.VMEM((group, FIELDS, rows), F32),
            pltpu.VMEM((group, FIELDS, rows), F32),
            pltpu.VMEM((FIELDS * depth, BLK), BF16),
            pltpu.VMEM((BLK + 2 * TAIL, FIELDS * depth), BF16),
            pltpu.VMEM((FIELDS, depth), F32),
            pltpu.VMEM((TAIL, BLK), F32),
            pltpu.VMEM((nz, HALF + TAIL, BLK), F32),
            pltpu.VMEM((nz - 1, HALF + TAIL, BLK), F32),
            pltpu.VMEM(args[1].shape, F32),
            pltpu.VMEM(args[4].shape, F32),
            pltpu.VMEM(args[5].shape, jnp.int32),
            pltpu.VMEM(args[6].shape, jnp.int32),
            pltpu.VMEM((nz * nc, 1, BLK), F32),
            pltpu.VMEM((nx * ny, 2, BLK), F32),
            dma, dma((4,)), dma((nz,)), dma, dma((2,)), dma((2,)),
            dma, dma, dma, dma, dma, dma,
        ],
        compiler_params=pltpu.CompilerParams(collective_id=0, has_side_effects=True),
    )(*args)
    return (scores[0], scores[1])


def solution(mesh):
    nx = mesh.shape["gene"]
    sizes = (4, 8, 2, nx)
    torus = Mesh(mesh.devices.reshape(sizes), ("y", "z", "c", "x"))
    samp = ("y", "z", "c")
    placed = (P(samp, "x"), P("x"), P(None, samp), P(None, samp), P("x"), P(), P())
    step = functools.partial(local, sizes)
    return jax.shard_map(step, mesh=torus, in_specs=placed, out_specs=(P(), P()), check_vma=False)
```

```python
import functools

import jax
import jax.numpy as jnp
from jax import lax
from jax.experimental import pallas as pl
from jax.experimental.pallas import tpu as pltpu
from jax.sharding import Mesh
from jax.sharding import PartitionSpec as P

BLK = 128
HALF = BLK // 2
FIELDS = 16
MESH = pl.DeviceIdType.MESH
F32 = jnp.float32
BF16 = jnp.bfloat16
TAIL = 8


def total(x):
    return jnp.sum(jnp.sum(x, axis=1, keepdims=True), axis=0, keepdims=True)


def masked(words, k):
    if k == FIELDS - 1:
        words, k = jnp.right_shift(words, 2), k - 1
    return jnp.bitwise_and(words, 3 << (2 * k)).astype(F32)


def kernel(
    sizes, genotypes, freq, weight, residual, variant_weight, block_gene, gene_variants, out,
    staged, words, side_staged, side_in, rhs, lhs, scale, tail, part, gathered, freq_v, vw_v, bg_v, gv_v,
    rows_one, rows_two, stage_sem, side_sem, small_sem, word_recv, word_send, side_recv, side_send,
    part_recv, part_send, one_recv, one_send, two_recv, two_send,
):
    ny, nz, nc, nx = sizes
    rows = genotypes.shape[0]
    depth = ny * nc * rows
    genes_here = nz * nc // 2
    y, z, c, x = (lax.axis_index(a) for a in ("y", "z", "c", "x"))
    mine = y * nc + c

    side_copies = [
        pltpu.make_async_copy(src, side_staged.at[i], side_sem.at[i])
        for i, src in enumerate((weight, residual))
    ]
    for copy in side_copies:
        copy.start()
    stage = pltpu.make_async_copy(genotypes, staged, stage_sem)
    stage.start()
    smalls = [
        pltpu.make_async_copy(src, dst, small_sem.at[i])
        for i, (src, dst) in enumerate(
            ((freq, freq_v), (variant_weight, vw_v), (block_gene, bg_v), (gene_variants, gv_v))
        )
    ]
    for copy in smalls:
        copy.start()

    def near(dy, dc):
        return (lax.rem(y + dy, ny), z, lax.rem(c + dc, nc), x)

    def along(dz, dc):
        return (y, lax.rem(z + dz, nz), lax.rem(c + dc, nc), x)

    def across(dx, dy):
        return (lax.rem(y + dy, ny), z, c, lax.rem(x + dx, nx))

    order = sorted(range(1, ny), key=lambda d: -min(d, ny - d))
    near_peers = [(dy, dc) for dy in order + [0] for dc in range(nc) if (dy, dc) != (0, 0)]
    along_peers = [(dz, dc) for dz in range(nz) for dc in range(nc) if (dz, dc) != (0, 0)]
    across_peers = [(dx, dy) for dx in range(nx) for dy in range(ny) if (dx, dy) != (0, 0)]
    greeted = [near(*p) for p in near_peers]
    greeted += [along(*p) for p in along_peers if p[0] != 0]
    greeted += [across(*p) for p in across_peers if p[0] != 0]
    barrier = pltpu.get_barrier_semaphore()
    for peer in greeted:
        pl.semaphore_signal(barrier, inc=1, device_id=peer, device_id_type=MESH)
    pl.semaphore_wait(barrier, len(greeted))

    for copy in side_copies:
        copy.wait()
    for peer in near_peers:
        pltpu.make_async_remote_copy(
            src_ref=side_staged, dst_ref=side_in.at[mine], send_sem=side_send, recv_sem=side_recv,
            device_id=near(*peer), device_id_type=MESH,
        ).start()
    for i, src in enumerate((weight, residual)):
        pltpu.make_async_copy(src, side_in.at[mine, i], side_recv).start()

    def owner_of(j, core):
        distance = nz // 2 - (j + 1) // 2
        sign = (2 * (j % 2) - 1) * (1 - 2 * core)
        return lax.rem(z + sign * distance + nz, nz)

    stage.wait()

    def send_words(j, carry):
        for dy, dc in near_peers:
            to = near(dy, dc)
            column = pl.multiple_of(((to[0] * nz + owner_of(j, to[2])) * nc + to[2]) * BLK, BLK)
            pltpu.make_async_remote_copy(
                src_ref=staged.at[:, pl.ds(column, BLK)], dst_ref=words.at[j, mine],
                send_sem=word_send, recv_sem=word_recv.at[j],
                device_id=to, device_id_type=MESH,
            ).start()
        column = pl.multiple_of(((y * nz + owner_of(j, c)) * nc + c) * BLK, BLK)
        pltpu.make_async_copy(
            genotypes.at[:, pl.ds(column, BLK)], words.at[j, mine], word_recv.at[j]
        ).start()
        return carry

    lax.fori_loop(0, nz, send_words, 0)

    pltpu.make_async_copy(side_in, side_in, side_recv).wait()
    weight_all, residual_all = (
        jnp.concatenate([side_in[g, i] for g in range(ny * nc)], axis=1) for i in range(2)
    )
    rounded = weight_all.astype(BF16).astype(F32)
    cross = weight_all * residual_all
    high = cross.astype(BF16).astype(F32)
    low = (cross - high).astype(BF16).astype(F32)
    field = lax.broadcasted_iota(jnp.int32, (FIELDS, 1), 0)
    inverse = jnp.ones((FIELDS, 1), F32)
    for k in range(1, FIELDS):
        inverse = jnp.where(field == k, 0.25 ** min(k, FIELDS - 2), inverse)
    scale[...] = rounded * (inverse * inverse)
    extra = [a * inverse for a in (rounded, high, low)]
    row_id = lax.broadcasted_iota(jnp.int32, (2 * TAIL, depth), 0)
    for k in range(FIELDS):
        rows_k = jnp.zeros((2 * TAIL, depth), F32)
        for i, a in enumerate(extra):
            rows_k = jnp.where(row_id == i, a[k : k + 1], rows_k)
        lhs[BLK : BLK + 2 * TAIL, k * depth : (k + 1) * depth] = rows_k.astype(BF16)
    sums = (total(rounded), total(high + low), total(cross * residual_all))
    lane = lax.broadcasted_iota(jnp.int32, (TAIL, BLK), 1)
    sublane = lax.broadcasted_iota(jnp.int32, (TAIL, BLK), 0)
    tail_rows = jnp.zeros((TAIL, BLK), F32)
    for i, s in enumerate(sums):
        tail_rows = jnp.where(sublane == 3 + i, s, tail_rows)
    tail[...] = tail_rows
    fold_down = lax.broadcasted_iota(jnp.int32, (HALF, BLK), 0)
    fold_side = lax.broadcasted_iota(jnp.int32, (HALF, BLK), 1)
    folded = jnp.logical_and(fold_side >= HALF, fold_down >= fold_side - HALF)

    def partial(j):
        pltpu.make_async_copy(words.at[j], words.at[j], word_recv.at[j]).wait()
        block = words[j].reshape(depth, BLK)
        turned = jnp.transpose(block)
        for k in range(FIELDS):
            rhs[k * depth : (k + 1) * depth, :] = masked(block, k).astype(BF16)
            lhs[:BLK, k * depth : (k + 1) * depth] = (masked(turned, k) * scale[k : k + 1, :]).astype(BF16)
        gram = jnp.dot(lhs[...], rhs[...], preferred_element_type=F32)
        low_rows = gram[HALF:BLK]
        part[j, :HALF] = jnp.where(folded, pltpu.roll(gram[:HALF], HALF, 1), low_rows)
        corner = jnp.sum(jnp.where(fold_side - HALF == fold_down, low_rows, 0.0), axis=0, keepdims=True)
        part[j, HALF:] = gram[BLK : BLK + TAIL] + jnp.where(sublane == 6, corner, tail[...])

    def far_block(j, carry):
        partial(j)
        pltpu.make_async_remote_copy(
            src_ref=part.at[j], dst_ref=gathered.at[j], send_sem=part_send, recv_sem=part_recv,
            device_id=(y, owner_of(j, c), c, x), device_id_type=MESH,
        ).start()
        return carry

    lax.fori_loop(0, nz - 1, far_block, 0)
    partial(nz - 1)

    for copy in smalls:
        copy.wait()
    own = (y * nz + z) * nc + c
    doubled = 2.0 * freq_v[pl.ds(own, 1), :]
    own_block = x * (ny * nz * nc) + own
    bg = bg_v[...]
    block_id = lax.broadcasted_iota(jnp.int32, bg.shape, 0) * BLK + lax.broadcasted_iota(jnp.int32, bg.shape, 1)
    gene = total(jnp.where(block_id == own_block, bg, 0))
    first = total((bg < gene).astype(jnp.int32))
    row_lane = lax.broadcasted_iota(jnp.int32, (1, BLK), 1)
    counted = total(jnp.where(row_lane == gene, gv_v[...], 0))
    live = (own_block - first) * BLK + row_lane < counted
    effective = jnp.where(live, vw_v[pl.ds(own, 1), :], 0.0)

    pltpu.make_async_copy(gathered, gathered, part_recv).wait()
    summed = part[nz - 1]
    for j in range(nz - 1):
        summed = summed + gathered[j]
    ends = summed[HALF:]
    linear, weight_sum = ends[0:1], ends[3:4]
    score = ends[1:2] + ends[2:3] - doubled * ends[4:5]
    down = lax.broadcasted_iota(jnp.int32, (BLK, BLK), 0)
    stacked = jnp.where(down == 0, doubled, jnp.where(down == 1, linear, jnp.where(down == 2, effective, 0.0)))
    upright = jnp.transpose(stacked)

    def by_row(i):
        return jnp.where(folded, upright[:HALF, i : i + 1], upright[HALF:, i : i + 1])

    def by_lane(row):
        return jnp.where(folded, pltpu.roll(row, HALF, 1), row)

    doubled_v, linear_v = by_lane(doubled), by_lane(linear)
    gram = summed[:HALF] - by_row(0) * (linear_v - doubled_v * weight_sum) - by_row(1) * doubled_v
    scaled = by_row(2) * gram * by_lane(effective)
    first_diagonal = fold_side - HALF == fold_down
    twice = jnp.where(first_diagonal, 1.0, 2.0) * scaled
    corner = ends[6:7] - doubled * (2.0 * linear - doubled * weight_sum)
    corner = jnp.where(row_lane >= HALF, effective * effective * corner, 0.0)
    weighted_score = effective * score
    stats = (
        total(weighted_score),
        total(twice) + total(corner),
        total(weighted_score * weighted_score),
        total(jnp.where(first_diagonal, scaled, 0.0)) + total(corner),
        total(twice * scaled) + total(corner * corner),
    )
    near_gene = gene - (x * ny + y) * genes_here
    row = jnp.zeros((1, BLK), F32)
    for i, s in enumerate(stats):
        row = jnp.where(row_lane == i * genes_here + near_gene, s, row)
    at_variance = len(stats) * genes_here
    share = jnp.where(c == 0, tail[5:6, :], 0.0)
    row = jnp.where(row_lane == at_variance, share, row)
    seat = z * nc + c
    rows_one[seat] = row
    for peer in along_peers:
        pltpu.make_async_remote_copy(
            src_ref=rows_one.at[seat], dst_ref=rows_one.at[seat], send_sem=one_send, recv_sem=one_recv,
            device_id=along(*peer), device_id_type=MESH,
        ).start()
    count = nz * nc - 1
    pltpu.make_async_copy(rows_one.at[pl.ds(0, count)], rows_one.at[pl.ds(0, count)], one_recv).wait()
    genes = rows_one[0]
    for i in range(1, count + 1):
        genes = genes + rows_one[i]

    place = x * ny + y
    samples = depth * nz * FIELDS
    variance = total(jnp.where(row_lane == at_variance, genes, 0.0)) / samples
    totals = [
        pltpu.roll(genes, lax.rem(place * genes_here - i * genes_here + BLK, BLK), 1)
        for i in range(len(stats))
    ]
    here = jnp.logical_and(row_lane >= place * genes_here, row_lane < (place + 1) * genes_here)
    totals = [jnp.where(here, t, 1.0) for t in totals]
    burden = totals[0] / jnp.sqrt(variance * totals[1])
    skat = (totals[2] - variance * totals[3]) / (variance * jnp.sqrt(2.0 * totals[4]))
    pair_row = lax.broadcasted_iota(jnp.int32, (2, BLK), 0)
    rows_two[place] = jnp.where(here, jnp.where(pair_row == 0, burden, skat), 0.0)
    for peer in across_peers:
        pltpu.make_async_remote_copy(
            src_ref=rows_two.at[place], dst_ref=rows_two.at[place], send_sem=two_send, recv_sem=two_recv,
            device_id=across(*peer), device_id_type=MESH,
        ).start()
    count = nx * ny - 1
    pltpu.make_async_copy(rows_two.at[pl.ds(0, count)], rows_two.at[pl.ds(0, count)], two_recv).wait()
    scores = rows_two[0]
    for i in range(1, count + 1):
        scores = scores + rows_two[i]
    out[...] = scores

    sent = len(near_peers)
    span = side_in.at[pl.ds(0, sent)]
    pltpu.make_async_copy(span, span, side_send).wait()
    span = words.at[:, pl.ds(0, sent)]
    pltpu.make_async_copy(span, span, word_send).wait()
    pltpu.make_async_copy(gathered, gathered, part_send).wait()
    span = rows_one.at[pl.ds(0, len(along_peers))]
    pltpu.make_async_copy(span, span, one_send).wait()
    span = rows_two.at[pl.ds(0, len(across_peers))]
    pltpu.make_async_copy(span, span, two_send).wait()


def local(
    sizes, genotypes, allele_freq, sample_weight, residual, variant_weight, block_gene, gene_variants
):
    ny, nz, nc, nx = sizes
    rows, columns = genotypes.shape
    group = ny * nc
    depth = group * rows
    blocks = columns // BLK
    args = (
        genotypes,
        allele_freq.reshape(blocks, BLK),
        sample_weight,
        residual,
        variant_weight.reshape(blocks, BLK),
        block_gene.reshape(-1, BLK),
        gene_variants.reshape(1, -1),
    )
    anywhere = pl.BlockSpec(memory_space=pl.ANY)
    dma = pltpu.SemaphoreType.DMA
    scores = pl.pallas_call(
        functools.partial(kernel, sizes),
        out_shape=pltpu.VMEM((2, BLK), F32),
        in_specs=[anywhere] * len(args),
        out_specs=pl.BlockSpec(memory_space=pltpu.VMEM),
        scratch_shapes=[
            pltpu.VMEM((rows, columns), jnp.int32),
            pltpu.VMEM((nz, group, rows, BLK), jnp.int32),
            pltpu.VMEM((2, FIELDS, rows), F32),
            pltpu.VMEM((group, 2, FIELDS, rows), F32),
            pltpu.VMEM((FIELDS * depth, BLK), BF16),
            pltpu.VMEM((BLK + 2 * TAIL, FIELDS * depth), BF16),
            pltpu.VMEM((FIELDS, depth), F32),
            pltpu.VMEM((TAIL, BLK), F32),
            pltpu.VMEM((nz, HALF + TAIL, BLK), F32),
            pltpu.VMEM((nz - 1, HALF + TAIL, BLK), F32),
            pltpu.VMEM(args[1].shape, F32),
            pltpu.VMEM(args[4].shape, F32),
            pltpu.VMEM(args[5].shape, jnp.int32),
            pltpu.VMEM(args[6].shape, jnp.int32),
            pltpu.VMEM((nz * nc, 1, BLK), F32),
            pltpu.VMEM((nx * ny, 2, BLK), F32),
            dma, dma((2,)), dma((4,)), dma((nz,)), dma, dma, dma,
            dma, dma, dma, dma, dma, dma,
        ],
        compiler_params=pltpu.CompilerParams(collective_id=0, has_side_effects=True),
    )(*args)
    return (scores[0], scores[1])


def solution(mesh):
    nx = mesh.shape["gene"]
    sizes = (4, 8, 2, nx)
    torus = Mesh(mesh.devices.reshape(sizes), ("y", "z", "c", "x"))
    samp = ("y", "z", "c")
    placed = (P(samp, "x"), P("x"), P(None, samp), P(None, samp), P("x"), P(), P())
    step = functools.partial(local, sizes)
    return jax.shard_map(step, mesh=torus, in_specs=placed, out_specs=(P(), P()), check_vma=False)
```

```python
import functools
import itertools

import jax
import jax.numpy as jnp
from jax import lax
from jax.experimental import pallas as pl
from jax.experimental.pallas import tpu as pltpu
from jax.sharding import Mesh
from jax.sharding import PartitionSpec as P

BLK = 128
HALF = BLK // 2
FIELDS = 16
MESH = pl.DeviceIdType.MESH
F32 = jnp.float32
BF16 = jnp.bfloat16
TAIL = 8


def total(x):
    return jnp.sum(jnp.sum(x, axis=1, keepdims=True), axis=0, keepdims=True)


def masked(words, k):
    if k == FIELDS - 1:
        words, k = jnp.right_shift(words, 2), k - 1
    return jnp.bitwise_and(words, 3 << (2 * k)).astype(F32)


def kernel(
    sizes, genotypes, freq, weight, residual, variant_weight, block_gene, gene_variants, out,
    staged, words, side_staged, side_in, rhs, lhs, scale, tail, part, gathered, freq_v, vw_v, bg_v, gv_v,
    rows_one, rows_two, rows_all, stage_sem, side_sem, small_sem, word_recv, word_send, side_recv, side_send,
    part_recv, part_send, one_recv, one_send, two_recv, two_send, row_recv, row_send,
):
    ny, nz, nc, nx = sizes
    rows = genotypes.shape[0]
    depth = ny * nc * rows
    genes_here = nz * nc // 2
    y, z, c, x = (lax.axis_index(a) for a in ("y", "z", "c", "x"))
    mine = y * nc + c

    side_copies = [
        pltpu.make_async_copy(src, side_staged.at[i], side_sem.at[i])
        for i, src in enumerate((weight, residual))
    ]
    for copy in side_copies:
        copy.start()
    stage = pltpu.make_async_copy(genotypes, staged, stage_sem)
    stage.start()
    smalls = [
        pltpu.make_async_copy(src, dst, small_sem.at[i])
        for i, (src, dst) in enumerate(
            ((freq, freq_v), (variant_weight, vw_v), (block_gene, bg_v), (gene_variants, gv_v))
        )
    ]
    for copy in smalls:
        copy.start()

    def near(dy, dc):
        return (lax.rem(y + dy, ny), z, lax.rem(c + dc, nc), x)

    def along(dz, core):
        return (y, lax.rem(z + dz, nz), core, x)

    def across(dx, dy, core):
        return (lax.rem(y + dy, ny), z, core, lax.rem(x + dx, nx))

    head = nc - 1
    order = sorted(range(1, ny), key=lambda d: -min(d, ny - d))
    near_peers = [(dy, dc) for dy in order + [0] for dc in range(nc) if (dy, dc) != (0, 0)]
    far_x = [(dx, dy) for dx in range(1, nx) for dy in range(ny)]
    barrier = pltpu.get_barrier_semaphore()

    def greet(peers):
        for peer in peers:
            pl.semaphore_signal(barrier, inc=1, device_id=peer, device_id_type=MESH)

    greet([near(*p) for p in near_peers])
    greet([along(dz, c) for dz in range(1, nz)])
    greet([across(*p, head) for p in far_x])

    @pl.when(c == head)
    def _():
        greet([along(dz, core) for dz in range(1, nz) for core in range(nc) if core != head])

    is_first = jnp.logical_and(x + y + z == 0, c == head)

    def known(y, z, c, x):
        return (x == 0) & ((z == 0) | (y == 0)) | (z == 0) & (c == head)

    @pl.when(is_first)
    def _():
        for to in itertools.product(range(ny), range(nz), range(nc), range(nx)):
            if not known(*to):
                greet([to])

    at_head = len(near_peers) + nz - 1 + len(far_x) * nc
    elsewhere = len(near_peers) + (nz - 1) * 2
    pl.semaphore_wait(barrier, jnp.where(c == head, at_head, elsewhere) + jnp.where(known(y, z, c, x), 0, 1))

    for copy in side_copies:
        copy.wait()
    for peer in near_peers:
        pltpu.make_async_remote_copy(
            src_ref=side_staged, dst_ref=side_in.at[mine], send_sem=side_send, recv_sem=side_recv,
            device_id=near(*peer), device_id_type=MESH,
        ).start()
    for i, src in enumerate((weight, residual)):
        pltpu.make_async_copy(src, side_in.at[mine, i], side_recv).start()

    def outward(core):
        middle = nz // 2
        return jnp.where(z < middle, 1, jnp.where(z > middle, -1, 1 - 2 * core))

    def owner_of(j, core):
        distance = nz // 2 - (j + 1) // 2
        sign = (2 * (j % 2) - 1) * outward(core)
        return lax.rem(z + sign * distance + nz, nz)

    stage.wait()

    def send_words(j, carry):
        for dy, dc in near_peers:
            to = near(dy, dc)
            column = pl.multiple_of(((to[0] * nz + owner_of(j, to[2])) * nc + to[2]) * BLK, BLK)
            pltpu.make_async_remote_copy(
                src_ref=staged.at[:, pl.ds(column, BLK)], dst_ref=words.at[j, mine],
                send_sem=word_send, recv_sem=word_recv.at[j],
                device_id=to, device_id_type=MESH,
            ).start()
        column = pl.multiple_of(((y * nz + owner_of(j, c)) * nc + c) * BLK, BLK)
        pltpu.make_async_copy(
            genotypes.at[:, pl.ds(column, BLK)], words.at[j, mine], word_recv.at[j]
        ).start()
        return carry

    lax.fori_loop(0, nz, send_words, 0)

    pltpu.make_async_copy(side_in, side_in, side_recv).wait()
    weight_all, residual_all = (
        jnp.concatenate([side_in[g, i] for g in range(ny * nc)], axis=1) for i in range(2)
    )
    rounded = weight_all.astype(BF16).astype(F32)
    cross = weight_all * residual_all
    high = cross.astype(BF16).astype(F32)
    low = (cross - high).astype(BF16).astype(F32)
    field = lax.broadcasted_iota(jnp.int32, (FIELDS, 1), 0)
    inverse = jnp.ones((FIELDS, 1), F32)
    for k in range(1, FIELDS):
        inverse = jnp.where(field == k, 0.25 ** min(k, FIELDS - 2), inverse)
    scale[...] = rounded * (inverse * inverse)
    extra = [a * inverse for a in (rounded, high, low)]
    row_id = lax.broadcasted_iota(jnp.int32, (2 * TAIL, depth), 0)
    for k in range(FIELDS):
        rows_k = jnp.zeros((2 * TAIL, depth), F32)
        for i, a in enumerate(extra):
            rows_k = jnp.where(row_id == i, a[k : k + 1], rows_k)
        lhs[BLK : BLK + 2 * TAIL, k * depth : (k + 1) * depth] = rows_k.astype(BF16)
    sums = (total(rounded), total(high + low), total(cross * residual_all))
    lane = lax.broadcasted_iota(jnp.int32, (TAIL, BLK), 1)
    sublane = lax.broadcasted_iota(jnp.int32, (TAIL, BLK), 0)
    tail_rows = jnp.zeros((TAIL, BLK), F32)
    for i, s in enumerate(sums):
        tail_rows = jnp.where(sublane == 3 + i, s, tail_rows)
    tail[...] = tail_rows
    fold_down = lax.broadcasted_iota(jnp.int32, (HALF, BLK), 0)
    fold_side = lax.broadcasted_iota(jnp.int32, (HALF, BLK), 1)
    folded = jnp.logical_and(fold_side >= HALF, fold_down >= fold_side - HALF)

    def partial(j):
        pltpu.make_async_copy(words.at[j], words.at[j], word_recv.at[j]).wait()
        block = words[j].reshape(depth, BLK)
        turned = jnp.transpose(block)
        for k in range(FIELDS):
            rhs[k * depth : (k + 1) * depth, :] = masked(block, k).astype(BF16)
            lhs[:BLK, k * depth : (k + 1) * depth] = (masked(turned, k) * scale[k : k + 1, :]).astype(BF16)
        gram = jnp.dot(lhs[...], rhs[...], preferred_element_type=F32)
        low_rows = gram[HALF:BLK]
        part[j, :HALF] = jnp.where(folded, pltpu.roll(gram[:HALF], HALF, 1), low_rows)
        corner = jnp.sum(jnp.where(fold_side - HALF == fold_down, low_rows, 0.0), axis=0, keepdims=True)
        part[j, HALF:] = gram[BLK : BLK + TAIL] + jnp.where(sublane == 6, corner, tail[...])

    def far_block(j, carry):
        partial(j)
        owner = owner_of(j, c)
        pltpu.make_async_remote_copy(
            src_ref=part.at[j], dst_ref=gathered.at[lax.rem(owner - z + nz, nz) - 1], send_sem=part_send, recv_sem=part_recv,
            device_id=(y, owner, c, x), device_id_type=MESH,
        ).start()
        return carry

    lax.fori_loop(0, nz - 1, far_block, 0)
    partial(nz - 1)

    for copy in smalls:
        copy.wait()
    own = (y * nz + z) * nc + c
    doubled = 2.0 * freq_v[pl.ds(own, 1), :]
    own_block = x * (ny * nz * nc) + own
    bg = bg_v[...]
    block_id = lax.broadcasted_iota(jnp.int32, bg.shape, 0) * BLK + lax.broadcasted_iota(jnp.int32, bg.shape, 1)
    gene = total(jnp.where(block_id == own_block, bg, 0))
    first = total((bg < gene).astype(jnp.int32))
    row_lane = lax.broadcasted_iota(jnp.int32, (1, BLK), 1)
    counted = total(jnp.where(row_lane == gene, gv_v[...], 0))
    live = (own_block - first) * BLK + row_lane < counted
    effective = jnp.where(live, vw_v[pl.ds(own, 1), :], 0.0)

    pltpu.make_async_copy(gathered, gathered, part_recv).wait()
    summed = part[nz - 1]
    for j in range(nz - 1):
        summed = summed + gathered[j]
    ends = summed[HALF:]
    linear, weight_sum = ends[0:1], ends[3:4]
    score = ends[1:2] + ends[2:3] - doubled * ends[4:5]
    down = lax.broadcasted_iota(jnp.int32, (BLK, BLK), 0)
    stacked = jnp.where(down == 0, doubled, jnp.where(down == 1, linear, jnp.where(down == 2, effective, 0.0)))
    upright = jnp.transpose(stacked)

    def by_row(i):
        return jnp.where(folded, upright[:HALF, i : i + 1], upright[HALF:, i : i + 1])

    def by_lane(row):
        return jnp.where(folded, pltpu.roll(row, HALF, 1), row)

    doubled_v, linear_v = by_lane(doubled), by_lane(linear)
    gram = summed[:HALF] - by_row(0) * (linear_v - doubled_v * weight_sum) - by_row(1) * doubled_v
    scaled = by_row(2) * gram * by_lane(effective)
    first_diagonal = fold_side - HALF == fold_down
    twice = jnp.where(first_diagonal, 1.0, 2.0) * scaled
    corner = ends[6:7] - doubled * (2.0 * linear - doubled * weight_sum)
    corner = jnp.where(row_lane >= HALF, effective * effective * corner, 0.0)
    weighted_score = effective * score
    stats = (
        total(weighted_score),
        total(twice) + total(corner),
        total(weighted_score * weighted_score),
        total(jnp.where(first_diagonal, scaled, 0.0)) + total(corner),
        total(twice * scaled) + total(corner * corner),
    )
    near_gene = gene - (x * ny + y) * genes_here
    row = jnp.zeros((1, BLK), F32)
    for i, s in enumerate(stats):
        row = jnp.where(row_lane == i * genes_here + near_gene, s, row)
    at_variance = len(stats) * genes_here
    share = jnp.where(c == 0, tail[5:6, :], 0.0)
    row = jnp.where(row_lane == at_variance, share, row)
    seat = z * nc + c
    place = x * ny + y
    group = nz * nc
    places = nx * ny
    samples = depth * nz * FIELDS
    rows_one[seat] = row

    @pl.when(place != 0)
    def _():
        pltpu.make_async_remote_copy(
            src_ref=rows_one.at[seat], dst_ref=rows_all.at[place * group + seat], send_sem=row_send, recv_sem=row_recv,
            device_id=(0, 0, head, 0), device_id_type=MESH,
        ).start()

    def send_row(dz):
        pltpu.make_async_remote_copy(
            src_ref=rows_one.at[seat], dst_ref=rows_one.at[seat], send_sem=one_send, recv_sem=one_recv,
            device_id=along(dz, head), device_id_type=MESH,
        ).start()

    for dz in range(1, nz):
        send_row(dz)

    @pl.when(c != head)
    def _():
        send_row(0)

    def added(rows_ref, base):
        genes = rows_ref[base]
        for i in range(1, group):
            genes = genes + rows_ref[base + i]
        return genes

    def scored(genes):
        lane_id = lax.broadcasted_iota(jnp.int32, genes.shape, 1)
        variance = jnp.sum(jnp.where(lane_id == at_variance, genes, 0.0), axis=1, keepdims=True) / samples
        totals = [genes] + [pltpu.roll(genes, BLK - i * genes_here, 1) for i in range(1, len(stats))]
        here = lane_id < genes_here
        totals = [jnp.where(here, t, 1.0) for t in totals]
        burden = totals[0] / jnp.sqrt(variance * totals[1])
        skat = (totals[2] - variance * totals[3]) / (variance * jnp.sqrt(2.0 * totals[4]))
        return [jnp.where(here, a, 0.0) for a in (burden, skat)]

    def finish(first_rows):
        lane_id = lax.broadcasted_iota(jnp.int32, (places, BLK), 1)
        place_id = lax.broadcasted_iota(jnp.int32, (places, BLK), 0)
        genes = jnp.concatenate([first_rows] + [added(rows_all, p * group) for p in range(1, places)], axis=0)
        for i, spread in enumerate(scored(genes)):
            width = genes_here
            while width < BLK:
                spread = spread + pltpu.roll(spread, width, 1)
                width *= 2
            spread = jnp.where(lane_id // genes_here == place_id, spread, 0.0)
            out[i : i + 1] = jnp.sum(spread, axis=0, keepdims=True)

    def merge():
        scores = rows_two[0]
        for i in range(1, places):
            scores = scores + rows_two[i]
        out[...] = scores

    def two_wait(count, sem):
        span = rows_two.at[pl.ds(0, count)]
        pltpu.make_async_copy(span, span, sem).wait()

    with_first = jnp.logical_and(z == 0, c == head)
    across_peers = [(dx, dy) for dx in range(nx) for dy in range(ny)]

    @pl.when(c == head)
    def _():
        span = rows_one.at[pl.ds(0, group - 1)]
        pltpu.make_async_copy(span, span, one_recv).wait()
        own_genes = added(rows_one, 0)
        pair_row = lax.broadcasted_iota(jnp.int32, (2, BLK), 0)
        burden, skat = (pltpu.roll(a, place * genes_here, 1) for a in scored(own_genes))
        rows_two[place] = jnp.where(pair_row == 0, burden, skat)

        def send_scores(to):
            pltpu.make_async_remote_copy(
                src_ref=rows_two.at[place], dst_ref=rows_two.at[place], send_sem=two_send, recv_sem=two_recv,
                device_id=to, device_id_type=MESH,
            ).start()

        for core in range(nc):
            for dx, dy in across_peers[::-1]:
                to = across(dx, dy, core)
                if core != head:
                    send_scores(to)
                elif dx + dy > 0:
                    pl.when(jnp.logical_not(with_first & (to[0] + to[3] == 0)))(
                        functools.partial(send_scores, to)
                    )

        @pl.when(is_first)
        def _():
            span = rows_all.at[pl.ds(0, group * (places - 1))]
            pltpu.make_async_copy(span, span, row_recv).wait()
            finish(own_genes)

        @pl.when(jnp.logical_not(is_first))
        def _():
            two_wait(places - 1, two_recv)
            merge()

        skipped = with_first & jnp.logical_not(is_first)

        two_wait(places, two_send)
        pl.when(skipped)(lambda: two_wait(places - 2, two_send))
        pl.when(jnp.logical_not(skipped))(lambda: two_wait(places - 1, two_send))

    @pl.when(c != head)
    def _():
        two_wait(places, two_recv)
        merge()
        pltpu.make_async_copy(rows_one.at[0], rows_one.at[0], one_send).wait()

    sent = len(near_peers)
    span = side_in.at[pl.ds(0, sent)]
    pltpu.make_async_copy(span, span, side_send).wait()
    span = words.at[:, pl.ds(0, sent)]
    pltpu.make_async_copy(span, span, word_send).wait()
    pltpu.make_async_copy(gathered, gathered, part_send).wait()
    span = rows_one.at[pl.ds(0, nz - 1)]
    pltpu.make_async_copy(span, span, one_send).wait()

    @pl.when(place != 0)
    def _():
        pltpu.make_async_copy(rows_all.at[0], rows_all.at[0], row_send).wait()


def local(
    sizes, genotypes, allele_freq, sample_weight, residual, variant_weight, block_gene, gene_variants
):
    ny, nz, nc, nx = sizes
    rows, columns = genotypes.shape
    group = ny * nc
    depth = group * rows
    blocks = columns // BLK
    args = (
        genotypes,
        allele_freq.reshape(blocks, BLK),
        sample_weight,
        residual,
        variant_weight.reshape(blocks, BLK),
        block_gene.reshape(-1, BLK),
        gene_variants.reshape(1, -1),
    )
    anywhere = pl.BlockSpec(memory_space=pl.ANY)
    dma = pltpu.SemaphoreType.DMA
    scores = pl.pallas_call(
        functools.partial(kernel, sizes),
        out_shape=pltpu.VMEM((2, BLK), F32),
        in_specs=[anywhere] * len(args),
        out_specs=pl.BlockSpec(memory_space=pltpu.VMEM),
        scratch_shapes=[
            pltpu.VMEM((rows, columns), jnp.int32),
            pltpu.VMEM((nz, group, rows, BLK), jnp.int32),
            pltpu.VMEM((2, FIELDS, rows), F32),
            pltpu.VMEM((group, 2, FIELDS, rows), F32),
            pltpu.VMEM((FIELDS * depth, BLK), BF16),
            pltpu.VMEM((BLK + 2 * TAIL, FIELDS * depth), BF16),
            pltpu.VMEM((FIELDS, depth), F32),
            pltpu.VMEM((TAIL, BLK), F32),
            pltpu.VMEM((nz, HALF + TAIL, BLK), F32),
            pltpu.VMEM((nz - 1, HALF + TAIL, BLK), F32),
            pltpu.VMEM(args[1].shape, F32),
            pltpu.VMEM(args[4].shape, F32),
            pltpu.VMEM(args[5].shape, jnp.int32),
            pltpu.VMEM(args[6].shape, jnp.int32),
            pltpu.VMEM((nz * nc, 1, BLK), F32),
            pltpu.VMEM((nx * ny, 2, BLK), F32),
            pltpu.VMEM((nx * ny * nz * nc, 1, BLK), F32),
            dma, dma((2,)), dma((4,)), dma((nz,)), dma, dma, dma,
            dma, dma, dma, dma, dma, dma, dma, dma,
        ],
        compiler_params=pltpu.CompilerParams(collective_id=0, has_side_effects=True),
    )(*args)
    return (scores[0], scores[1])


def solution(mesh):
    nx = mesh.shape["gene"]
    sizes = (4, 8, 2, nx)
    torus = Mesh(mesh.devices.reshape(sizes), ("y", "z", "c", "x"))
    samp = ("y", "z", "c")
    placed = (P(samp, "x"), P("x"), P(None, samp), P(None, samp), P("x"), P(), P())
    step = functools.partial(local, sizes)
    return jax.shard_map(step, mesh=torus, in_specs=placed, out_specs=(P(), P()), check_vma=False)
```

```python
import functools
import itertools

import jax
import jax.numpy as jnp
from jax import lax
from jax.experimental import pallas as pl
from jax.experimental.pallas import tpu as pltpu
from jax.sharding import Mesh
from jax.sharding import PartitionSpec as P

BLK = 128
HALF = BLK // 2
FIELDS = 16
MESH = pl.DeviceIdType.MESH
F32 = jnp.float32
BF16 = jnp.bfloat16
TAIL = 8
LINE_AT = 2


def total(x):
    return jnp.sum(jnp.sum(x, axis=1, keepdims=True), axis=0, keepdims=True)


def masked(words, k):
    if k == FIELDS - 1:
        words, k = jnp.right_shift(words, 2), k - 1
    return jnp.bitwise_and(words, 3 << (2 * k)).astype(F32)


def kernel(
    sizes, genotypes, freq, weight, residual, variant_weight, block_gene, gene_variants, out,
    staged, words, side_staged, side_in, rhs, lhs, scale, tail, part, gathered, freq_v, vw_v, bg_v, gv_v,
    rows_one, rows_two, rows_all,
    line_side, line_words, line_rhs, line_lhs, line_scale, line_tail, line_part, line_in, result,
    line_side_recv, line_side_send, line_recv, line_send, line_part_recv, line_part_send, stage_sem, side_sem, small_sem, word_recv, word_send, side_recv, side_send,
    part_recv, part_send, one_recv, one_send, two_recv, two_send, row_recv, row_send,
):
    ny, nz, nc, nx = sizes
    rows = genotypes.shape[0]
    depth = ny * nc * rows
    genes_here = nz * nc // 2
    y, z, c, x = (lax.axis_index(a) for a in ("y", "z", "c", "x"))
    mine = y * nc + c

    side_copies = [
        pltpu.make_async_copy(src, side_staged.at[i], side_sem.at[i])
        for i, src in enumerate((weight, residual))
    ]
    for copy in side_copies:
        copy.start()
    stage = pltpu.make_async_copy(genotypes, staged, stage_sem)
    stage.start()
    smalls = [
        pltpu.make_async_copy(src, dst, small_sem.at[i])
        for i, (src, dst) in enumerate(
            ((freq, freq_v), (variant_weight, vw_v), (block_gene, bg_v), (gene_variants, gv_v))
        )
    ]
    for copy in smalls:
        copy.start()

    def near(dy, dc):
        return (lax.rem(y + dy, ny), z, lax.rem(c + dc, nc), x)

    def along(dz, core):
        return (y, lax.rem(z + dz, nz), core, x)

    def across(dx, dy, core):
        return (lax.rem(y + dy, ny), z, core, lax.rem(x + dx, nx))

    head = nc - 1
    order = sorted(range(1, ny), key=lambda d: -min(d, ny - d))
    near_peers = [(dy, dc) for dy in order + [0] for dc in range(nc) if (dy, dc) != (0, 0)]
    far_x = [(dx, dy) for dx in range(1, nx) for dy in range(ny)]
    barrier = pltpu.get_barrier_semaphore()

    def greet(peers):
        for peer in peers:
            pl.semaphore_signal(barrier, inc=1, device_id=peer, device_id_type=MESH)

    greet([near(*p) for p in near_peers])
    greet([along(dz, core) for dz in range(1, nz) for core in range(nc)])
    greet([across(*p, head) for p in far_x])

    is_first = jnp.logical_and(x + y + z == 0, c == head)

    far_steps = 1
    far_places = [
        px * ny + py for px in range(nx) for py in range(ny)
        if min(px, nx - px) + min(py, ny - py) >= far_steps
    ]
    is_far = functools.reduce(jnp.logical_or, [x * ny + y == p for p in far_places])

    def met(y, z, c, x):
        return (x == 0) & ((z == 0) | (y == 0)) | (z == 0) & (c == head)

    @pl.when(is_first)
    def _():
        for to in itertools.product(range(ny), range(nz), range(nc), range(nx)):
            if to[3] * ny + to[0] in far_places and not met(*to):
                greet([to])

    elsewhere = len(near_peers) + (nz - 1) * nc
    at_head = elsewhere + len(far_x) * nc
    pl.semaphore_wait(barrier, jnp.where(c == head, at_head, elsewhere) + jnp.where(is_far & jnp.logical_not(met(y, z, c, x)), 1, 0))

    for copy in side_copies:
        copy.wait()
    for peer in near_peers:
        pltpu.make_async_remote_copy(
            src_ref=side_staged, dst_ref=side_in.at[mine], send_sem=side_send, recv_sem=side_recv,
            device_id=near(*peer), device_id_type=MESH,
        ).start()
    for i, src in enumerate((weight, residual)):
        pltpu.make_async_copy(src, side_in.at[mine, i], side_recv).start()

    line = z * nc + c
    line_core = lax.rem(z, nc)
    takes_line = c == line_core
    owns_line = z == y * nc + c

    def line_target(dz):
        zo = lax.rem(z + dz, nz)
        return (y, zo, lax.rem(zo, nc), x)

    def line_column(dz):
        zo = lax.rem(z + dz, nz)
        return pl.multiple_of(((zo // nc * nz + zo) * nc + lax.rem(zo, nc)) * BLK, BLK)

    def send_side(dz):
        pltpu.make_async_remote_copy(
            src_ref=side_staged, dst_ref=line_side.at[line], send_sem=line_side_send, recv_sem=line_side_recv,
            device_id=line_target(dz), device_id_type=MESH,
        ).start()

    def send_line(dz):
        pltpu.make_async_remote_copy(
            src_ref=staged.at[:, pl.ds(line_column(dz), BLK)], dst_ref=line_words.at[line],
            send_sem=line_send, recv_sem=line_recv, device_id=line_target(dz), device_id_type=MESH,
        ).start()

    spread = sorted(range(1, nz), key=lambda d: -min(d, nz - d))
    for dz in spread:
        send_side(dz)

    @pl.when(takes_line)
    def _():
        for i, src in enumerate((weight, residual)):
            pltpu.make_async_copy(src, line_side.at[line, i], line_side_recv).start()
        pltpu.make_async_copy(genotypes.at[:, pl.ds(line_column(0), BLK)], line_words.at[line], line_recv).start()

    @pl.when(jnp.logical_not(takes_line))
    def _():
        send_side(0)

    stage.wait()
    for dz in spread:
        send_line(dz)
    pl.when(jnp.logical_not(takes_line))(lambda: send_line(0))

    def outward(core):
        middle = nz // 2
        return jnp.where(z < middle, 1, jnp.where(z > middle, -1, 1 - 2 * core))

    def owner_of(j, core):
        distance = nz // 2 - (j + 1) // 2
        sign = (2 * (j % 2) - 1) * outward(core)
        return lax.rem(z + sign * distance + nz, nz)

    def send_words(j, carry):
        def send(to):
            column = pl.multiple_of(((to[0] * nz + owner_of(j, to[2])) * nc + to[2]) * BLK, BLK)
            pltpu.make_async_remote_copy(
                src_ref=staged.at[:, pl.ds(column, BLK)], dst_ref=words.at[j, mine],
                send_sem=word_send, recv_sem=word_recv.at[j],
                device_id=to, device_id_type=MESH,
            ).start()

        for peer in near_peers:
            to = near(*peer)
            pl.when(owner_of(j, to[2]) != to[0] * nc + to[2])(functools.partial(send, to))

        @pl.when(owner_of(j, c) != mine)
        def _():
            column = pl.multiple_of(((y * nz + owner_of(j, c)) * nc + c) * BLK, BLK)
            pltpu.make_async_copy(
                genotypes.at[:, pl.ds(column, BLK)], words.at[j, mine], word_recv.at[j]
            ).start()

        return carry

    lax.fori_loop(0, nz, send_words, 0)

    lane = lax.broadcasted_iota(jnp.int32, (TAIL, BLK), 1)
    sublane = lax.broadcasted_iota(jnp.int32, (TAIL, BLK), 0)

    def prepare(side_ref, lhs_ref, scale_ref, tail_ref):
        count = side_ref.shape[0]
        width = count * rows
        weight_all, residual_all = (
            jnp.concatenate([side_ref[g, i] for g in range(count)], axis=1) for i in range(2)
        )
        rounded = weight_all.astype(BF16).astype(F32)
        cross = weight_all * residual_all
        high = cross.astype(BF16).astype(F32)
        low = (cross - high).astype(BF16).astype(F32)
        field = lax.broadcasted_iota(jnp.int32, (FIELDS, 1), 0)
        inverse = jnp.ones((FIELDS, 1), F32)
        for k in range(1, FIELDS):
            inverse = jnp.where(field == k, 0.25 ** min(k, FIELDS - 2), inverse)
        scale_ref[...] = rounded * (inverse * inverse)
        extra = [a * inverse for a in (rounded, high, low)]
        row_id = lax.broadcasted_iota(jnp.int32, (2 * TAIL, width), 0)
        for k in range(FIELDS):
            rows_k = jnp.zeros((2 * TAIL, width), F32)
            for i, a in enumerate(extra):
                rows_k = jnp.where(row_id == i, a[k : k + 1], rows_k)
            lhs_ref[BLK : BLK + 2 * TAIL, k * width : (k + 1) * width] = rows_k.astype(BF16)
        tail_rows = jnp.zeros((TAIL, BLK), F32)
        for i, s in enumerate((total(rounded), total(high + low), total(cross * residual_all))):
            tail_rows = jnp.where(sublane == 3 + i, s, tail_rows)
        tail_ref[...] = tail_rows

    pltpu.make_async_copy(side_in, side_in, side_recv).wait()
    prepare(side_in, lhs, scale, tail)

    @pl.when(takes_line)
    def _():
        pltpu.make_async_copy(line_side, line_side, line_side_recv).wait()
        prepare(line_side, line_lhs, line_scale, line_tail)

    fold_down = lax.broadcasted_iota(jnp.int32, (HALF, BLK), 0)
    fold_side = lax.broadcasted_iota(jnp.int32, (HALF, BLK), 1)
    folded = jnp.logical_and(fold_side >= HALF, fold_down >= fold_side - HALF)

    def reduce_block(block, lhs_ref, rhs_ref, scale_ref, tail_ref, to_ref):
        width = block.shape[0]
        turned = jnp.transpose(block)
        for k in range(FIELDS):
            at = slice(k * width, (k + 1) * width)
            rhs_ref[at, :] = masked(block, k).astype(BF16)
            lhs_ref[:BLK, at] = (masked(turned, k) * scale_ref[k : k + 1, :]).astype(BF16)
        gram = jnp.dot(lhs_ref[...], rhs_ref[...], preferred_element_type=F32)
        low_rows = gram[HALF:BLK]
        to_ref[:HALF] = jnp.where(folded, pltpu.roll(gram[:HALF], HALF, 1), low_rows)
        corner = jnp.sum(jnp.where(fold_side - HALF == fold_down, low_rows, 0.0), axis=0, keepdims=True)
        to_ref[HALF:] = gram[BLK : BLK + TAIL] + jnp.where(sublane == 6, corner, tail_ref[...])

    def partial(j):
        pltpu.make_async_copy(words.at[j], words.at[j], word_recv.at[j]).wait()
        reduce_block(words[j].reshape(depth, BLK), lhs, rhs, scale, tail, part.at[j])

    def far_block(j, carry):
        owner = owner_of(j, c)

        @pl.when(owner != mine)
        def _():
            partial(j)
            pltpu.make_async_remote_copy(
                src_ref=part.at[j], dst_ref=gathered.at[lax.rem(owner - z + nz, nz) - 1],
                send_sem=part_send, recv_sem=part_recv,
                device_id=(y, owner, c, x), device_id_type=MESH,
            ).start()

        return carry

    line_at = min(LINE_AT, nz - 1)
    lax.fori_loop(0, line_at, far_block, 0)

    @pl.when(takes_line)
    def _():
        pltpu.make_async_copy(line_words, line_words, line_recv).wait()
        block = line_words[...].reshape(nz * nc * rows, BLK)
        reduce_block(block, line_lhs, line_rhs, line_scale, line_tail, line_part)

        @pl.when(jnp.logical_not(owns_line))
        def _():
            pltpu.make_async_remote_copy(
                src_ref=line_part, dst_ref=line_in.at[y], send_sem=line_part_send, recv_sem=line_part_recv,
                device_id=(z // nc, z, c, x), device_id_type=MESH,
            ).start()

    lax.fori_loop(line_at, nz - 1, far_block, 0)
    pl.when(jnp.logical_not(owns_line))(lambda: partial(nz - 1))

    for copy in smalls:
        copy.wait()
    own = (y * nz + z) * nc + c
    doubled = 2.0 * freq_v[pl.ds(own, 1), :]
    own_block = x * (ny * nz * nc) + own
    bg = bg_v[...]
    block_id = lax.broadcasted_iota(jnp.int32, bg.shape, 0) * BLK + lax.broadcasted_iota(jnp.int32, bg.shape, 1)
    gene = total(jnp.where(block_id == own_block, bg, 0))
    first = total((bg < gene).astype(jnp.int32))
    row_lane = lax.broadcasted_iota(jnp.int32, (1, BLK), 1)
    counted = total(jnp.where(row_lane == gene, gv_v[...], 0))
    live = (own_block - first) * BLK + row_lane < counted
    effective = jnp.where(live, vw_v[pl.ds(own, 1), :], 0.0)

    @pl.when(owns_line)
    def _():
        span = line_in.at[pl.ds(0, ny - 1)]
        pltpu.make_async_copy(span, span, line_part_recv).wait()
        got = line_part[...]
        for dy in range(1, ny):
            got = got + line_in[lax.rem(y + dy, ny)]
        result[...] = got

    @pl.when(jnp.logical_not(owns_line))
    def _():
        pltpu.make_async_copy(gathered, gathered, part_recv).wait()
        got = part[nz - 1]
        for j in range(nz - 1):
            got = got + gathered[j]
        result[...] = got

    summed = result[...]
    ends = summed[HALF:]
    linear, weight_sum = ends[0:1], ends[3:4]
    score = ends[1:2] + ends[2:3] - doubled * ends[4:5]
    down = lax.broadcasted_iota(jnp.int32, (BLK, BLK), 0)
    stacked = jnp.where(down == 0, doubled, jnp.where(down == 1, linear, jnp.where(down == 2, effective, 0.0)))
    upright = jnp.transpose(stacked)

    def by_row(i):
        return jnp.where(folded, upright[:HALF, i : i + 1], upright[HALF:, i : i + 1])

    def by_lane(row):
        return jnp.where(folded, pltpu.roll(row, HALF, 1), row)

    doubled_v, linear_v = by_lane(doubled), by_lane(linear)
    gram = summed[:HALF] - by_row(0) * (linear_v - doubled_v * weight_sum) - by_row(1) * doubled_v
    scaled = by_row(2) * gram * by_lane(effective)
    first_diagonal = fold_side - HALF == fold_down
    twice = jnp.where(first_diagonal, 1.0, 2.0) * scaled
    corner = ends[6:7] - doubled * (2.0 * linear - doubled * weight_sum)
    corner = jnp.where(row_lane >= HALF, effective * effective * corner, 0.0)
    weighted_score = effective * score
    stats = (
        total(weighted_score),
        total(twice) + total(corner),
        total(weighted_score * weighted_score),
        total(jnp.where(first_diagonal, scaled, 0.0)) + total(corner),
        total(twice * scaled) + total(corner * corner),
    )
    near_gene = gene - (x * ny + y) * genes_here
    row = jnp.zeros((1, BLK), F32)
    for i, s in enumerate(stats):
        row = jnp.where(row_lane == i * genes_here + near_gene, s, row)
    at_variance = len(stats) * genes_here
    share = jnp.where(c == 0, tail[5:6, :], 0.0)
    row = jnp.where(row_lane == at_variance, share, row)
    seat = z * nc + c
    place = x * ny + y
    group = nz * nc
    places = nx * ny
    samples = depth * nz * FIELDS
    rows_one[seat] = row
    far_id = sum(i * (place == p).astype(jnp.int32) for i, p in enumerate(far_places))

    @pl.when(is_far)
    def _():
        pltpu.make_async_remote_copy(
            src_ref=rows_one.at[seat], dst_ref=rows_all.at[far_id * group + seat], send_sem=row_send, recv_sem=row_recv,
            device_id=(0, 0, head, 0), device_id_type=MESH,
        ).start()

    def send_row(dz):
        pltpu.make_async_remote_copy(
            src_ref=rows_one.at[seat], dst_ref=rows_one.at[seat], send_sem=one_send, recv_sem=one_recv,
            device_id=along(dz, head), device_id_type=MESH,
        ).start()

    for dz in range(1, nz):
        send_row(dz)

    @pl.when(c != head)
    def _():
        send_row(0)

    def added(rows_ref, base):
        genes = rows_ref[base]
        for i in range(1, group):
            genes = genes + rows_ref[base + i]
        return genes

    def scored(genes):
        lane_id = lax.broadcasted_iota(jnp.int32, genes.shape, 1)
        variance = jnp.sum(jnp.where(lane_id == at_variance, genes, 0.0), axis=1, keepdims=True) / samples
        totals = [genes] + [pltpu.roll(genes, BLK - i * genes_here, 1) for i in range(1, len(stats))]
        here = lane_id < genes_here
        totals = [jnp.where(here, t, 1.0) for t in totals]
        burden = totals[0] / jnp.sqrt(variance * totals[1])
        skat = (totals[2] - variance * totals[3]) / (variance * jnp.sqrt(2.0 * totals[4]))
        return [jnp.where(here, a, 0.0) for a in (burden, skat)]

    def merge(chosen):
        scores = rows_two[chosen[0]]
        for p in chosen[1:]:
            scores = scores + rows_two[p]
        return scores

    def finish():
        genes = jnp.concatenate([added(rows_all, i * group) for i in range(len(far_places))], axis=0)
        lane_id = lax.broadcasted_iota(jnp.int32, genes.shape, 1)
        row_id = lax.broadcasted_iota(jnp.int32, genes.shape, 0)
        place_id = sum(jnp.where(row_id == i, p, 0) for i, p in enumerate(far_places))
        near_scores = merge([p for p in range(places) if p not in far_places])
        for i, spread in enumerate(scored(genes)):
            width = genes_here
            while width < BLK:
                spread = spread + pltpu.roll(spread, width, 1)
                width *= 2
            spread = jnp.where(lane_id // genes_here == place_id, spread, 0.0)
            out[i : i + 1] = near_scores[i : i + 1] + jnp.sum(spread, axis=0, keepdims=True)

    def two_wait(count, sem):
        span = rows_two.at[pl.ds(0, count)]
        pltpu.make_async_copy(span, span, sem).wait()

    with_first = jnp.logical_and(z == 0, c == head)
    across_peers = [(dx, dy) for dx in range(nx) for dy in range(ny)]

    @pl.when(c == head)
    def _():
        span = rows_one.at[pl.ds(0, group - 1)]
        pltpu.make_async_copy(span, span, one_recv).wait()
        own_genes = added(rows_one, 0)
        pair_row = lax.broadcasted_iota(jnp.int32, (2, BLK), 0)
        burden, skat = (pltpu.roll(a, place * genes_here, 1) for a in scored(own_genes))
        rows_two[place] = jnp.where(pair_row == 0, burden, skat)

        def send_scores(to):
            pltpu.make_async_remote_copy(
                src_ref=rows_two.at[place], dst_ref=rows_two.at[place], send_sem=two_send, recv_sem=two_recv,
                device_id=to, device_id_type=MESH,
            ).start()

        for core in range(nc):
            for dx, dy in across_peers[::-1]:
                to = across(dx, dy, core)
                if core != head:
                    send_scores(to)
                elif dx + dy > 0:
                    pl.when(jnp.logical_not(with_first & is_far & (to[0] + to[3] == 0)))(
                        functools.partial(send_scores, to)
                    )

        @pl.when(is_first)
        def _():
            if places - 1 > len(far_places):
                two_wait(places - 1 - len(far_places), two_recv)
            span = rows_all.at[pl.ds(0, group * len(far_places))]
            pltpu.make_async_copy(span, span, row_recv).wait()
            finish()

        @pl.when(jnp.logical_not(is_first))
        def _():
            two_wait(places - 1, two_recv)
            out[...] = merge(range(places))

        skipped = with_first & is_far

        two_wait(places, two_send)
        pl.when(skipped)(lambda: two_wait(places - 2, two_send))
        pl.when(jnp.logical_not(skipped))(lambda: two_wait(places - 1, two_send))

    @pl.when(c != head)
    def _():
        two_wait(places, two_recv)
        out[...] = merge(range(places))
        pltpu.make_async_copy(rows_one.at[0], rows_one.at[0], one_send).wait()

    sent = len(near_peers)
    span = side_in.at[pl.ds(0, sent)]
    pltpu.make_async_copy(span, span, side_send).wait()
    span = words.at[pl.ds(0, nz - 1), pl.ds(0, sent)]
    pltpu.make_async_copy(span, span, word_send).wait()

    def sent_line(count):
        for ref, sem in ((line_side, line_side_send), (line_words, line_send)):
            span = ref.at[pl.ds(0, count)]
            pltpu.make_async_copy(span, span, sem).wait()

    pl.when(takes_line)(lambda: sent_line(nz - 1))
    pl.when(jnp.logical_not(takes_line))(lambda: sent_line(nz))

    @pl.when(jnp.logical_and(takes_line, jnp.logical_not(owns_line)))
    def _():
        pltpu.make_async_copy(line_part, line_part, line_part_send).wait()

    def sent_parts(count):
        span = gathered.at[pl.ds(0, count)]
        pltpu.make_async_copy(span, span, part_send).wait()

    pl.when(owns_line)(lambda: sent_parts(nz - 1))
    pl.when(jnp.logical_not(owns_line))(lambda: sent_parts(nz - 2))
    span = rows_one.at[pl.ds(0, nz - 1)]
    pltpu.make_async_copy(span, span, one_send).wait()

    @pl.when(is_far)
    def _():
        pltpu.make_async_copy(rows_all.at[0], rows_all.at[0], row_send).wait()


def local(
    sizes, genotypes, allele_freq, sample_weight, residual, variant_weight, block_gene, gene_variants
):
    ny, nz, nc, nx = sizes
    rows, columns = genotypes.shape
    group = ny * nc
    depth = group * rows
    blocks = columns // BLK
    args = (
        genotypes,
        allele_freq.reshape(blocks, BLK),
        sample_weight,
        residual,
        variant_weight.reshape(blocks, BLK),
        block_gene.reshape(-1, BLK),
        gene_variants.reshape(1, -1),
    )
    anywhere = pl.BlockSpec(memory_space=pl.ANY)
    dma = pltpu.SemaphoreType.DMA
    scores = pl.pallas_call(
        functools.partial(kernel, sizes),
        out_shape=pltpu.VMEM((2, BLK), F32),
        in_specs=[anywhere] * len(args),
        out_specs=pl.BlockSpec(memory_space=pltpu.VMEM),
        scratch_shapes=[
            pltpu.VMEM((rows, columns), jnp.int32),
            pltpu.VMEM((nz, group, rows, BLK), jnp.int32),
            pltpu.VMEM((2, FIELDS, rows), F32),
            pltpu.VMEM((group, 2, FIELDS, rows), F32),
            pltpu.VMEM((FIELDS * depth, BLK), BF16),
            pltpu.VMEM((BLK + 2 * TAIL, FIELDS * depth), BF16),
            pltpu.VMEM((FIELDS, depth), F32),
            pltpu.VMEM((TAIL, BLK), F32),
            pltpu.VMEM((nz, HALF + TAIL, BLK), F32),
            pltpu.VMEM((nz - 1, HALF + TAIL, BLK), F32),
            pltpu.VMEM(args[1].shape, F32),
            pltpu.VMEM(args[4].shape, F32),
            pltpu.VMEM(args[5].shape, jnp.int32),
            pltpu.VMEM(args[6].shape, jnp.int32),
            pltpu.VMEM((nz * nc, 1, BLK), F32),
            pltpu.VMEM((nx * ny, 2, BLK), F32),
            pltpu.VMEM((nx * ny * nz * nc, 1, BLK), F32),
            pltpu.VMEM((nz * nc, 2, FIELDS, rows), F32),
            pltpu.VMEM((nz * nc, rows, BLK), jnp.int32),
            pltpu.VMEM((FIELDS * nz * nc * rows, BLK), BF16),
            pltpu.VMEM((BLK + 2 * TAIL, FIELDS * nz * nc * rows), BF16),
            pltpu.VMEM((FIELDS, nz * nc * rows), F32),
            pltpu.VMEM((TAIL, BLK), F32),
            pltpu.VMEM((HALF + TAIL, BLK), F32),
            pltpu.VMEM((ny, HALF + TAIL, BLK), F32),
            pltpu.VMEM((HALF + TAIL, BLK), F32),
            dma, dma, dma, dma, dma, dma,
            dma, dma((2,)), dma((4,)), dma((nz,)), dma, dma, dma,
            dma, dma, dma, dma, dma, dma, dma, dma,
        ],
        compiler_params=pltpu.CompilerParams(collective_id=0, has_side_effects=True),
    )(*args)
    return (scores[0], scores[1])


def solution(mesh):
    nx = mesh.shape["gene"]
    sizes = (4, 8, 2, nx)
    torus = Mesh(mesh.devices.reshape(sizes), ("y", "z", "c", "x"))
    samp = ("y", "z", "c")
    placed = (P(samp, "x"), P("x"), P(None, samp), P(None, samp), P("x"), P(), P())
    step = functools.partial(local, sizes)
    return jax.shard_map(step, mesh=torus, in_specs=placed, out_specs=(P(), P()), check_vma=False)
```

```python
import functools
import itertools

import jax
import jax.numpy as jnp
from jax import lax
from jax.experimental import pallas as pl
from jax.experimental.pallas import tpu as pltpu
from jax.sharding import Mesh
from jax.sharding import PartitionSpec as P

BLK = 128
HALF = BLK // 2
FIELDS = 16
MESH = pl.DeviceIdType.MESH
F32 = jnp.float32
BF16 = jnp.bfloat16
TAIL = 8
LINE_AT = 2


def total(x):
    return jnp.sum(jnp.sum(x, axis=1, keepdims=True), axis=0, keepdims=True)


def masked(words, k):
    if k == FIELDS - 1:
        words, k = jnp.right_shift(words, 2), k - 1
    return jnp.bitwise_and(words, 3 << (2 * k)).astype(F32)


def kernel(
    sizes, genotypes, freq, weight, residual, variant_weight, block_gene, gene_variants, out,
    staged, words, side_staged, side_in, rhs, lhs, scale, tail, part, gathered, freq_v, vw_v, bg_v, gv_v,
    rows_one, rows_two, rows_all,
    line_side, line_words, line_rhs, line_lhs, line_scale, line_tail, line_part, line_in, result,
    line_side_recv, line_side_send, line_recv, line_send, line_part_recv, line_part_send, stage_sem, side_sem, small_sem, word_recv, word_send, side_recv, side_send,
    part_recv, part_send, one_recv, one_send, two_recv, two_send, row_recv, row_send,
):
    ny, nz, nc, nx = sizes
    rows = genotypes.shape[0]
    depth = ny * nc * rows
    genes_here = nz * nc // 2
    y, z, c, x = (lax.axis_index(a) for a in ("y", "z", "c", "x"))
    mine = y * nc + c

    side_copies = [
        pltpu.make_async_copy(src, side_staged.at[i], side_sem.at[i])
        for i, src in enumerate((weight, residual))
    ]
    for copy in side_copies:
        copy.start()
    stage = pltpu.make_async_copy(genotypes, staged, stage_sem)
    stage.start()
    smalls = [
        pltpu.make_async_copy(src, dst, small_sem.at[i])
        for i, (src, dst) in enumerate(
            ((freq, freq_v), (variant_weight, vw_v), (block_gene, bg_v), (gene_variants, gv_v))
        )
    ]
    for copy in smalls:
        copy.start()

    def near(dy, dc):
        return (lax.rem(y + dy, ny), z, lax.rem(c + dc, nc), x)

    def along(dz, core):
        return (y, lax.rem(z + dz, nz), core, x)

    def across(dx, dy, core):
        return (lax.rem(y + dy, ny), z, core, lax.rem(x + dx, nx))

    head = nc - 1
    order = sorted(range(1, ny), key=lambda d: min(d, ny - d))
    near_peers = [(dy, dc) for dy in order + [0] for dc in range(nc) if (dy, dc) != (0, 0)]
    far_x = [(dx, dy) for dx in range(1, nx) for dy in range(ny)]
    barrier = pltpu.get_barrier_semaphore()

    def greet(peers):
        for peer in peers:
            pl.semaphore_signal(barrier, inc=1, device_id=peer, device_id_type=MESH)

    greet([near(*p) for p in near_peers])
    greet([along(dz, core) for dz in range(1, nz) for core in range(nc)])
    greet([across(*p, head) for p in far_x])

    is_first = jnp.logical_and(x + y + z == 0, c == head)

    far_steps = 1
    far_places = [
        px * ny + py for px in range(nx) for py in range(ny)
        if min(px, nx - px) + min(py, ny - py) >= far_steps
    ]
    is_far = functools.reduce(jnp.logical_or, [x * ny + y == p for p in far_places])

    def met(y, z, c, x):
        return (x == 0) & ((z == 0) | (y == 0)) | (z == 0) & (c == head)

    @pl.when(is_first)
    def _():
        for to in itertools.product(range(ny), range(nz), range(nc), range(nx)):
            if to[3] * ny + to[0] in far_places and not met(*to):
                greet([to])

    elsewhere = len(near_peers) + (nz - 1) * nc
    at_head = elsewhere + len(far_x) * nc
    pl.semaphore_wait(barrier, jnp.where(c == head, at_head, elsewhere) + jnp.where(is_far & jnp.logical_not(met(y, z, c, x)), 1, 0))

    for copy in side_copies:
        copy.wait()
    for peer in near_peers:
        pltpu.make_async_remote_copy(
            src_ref=side_staged, dst_ref=side_in.at[mine], send_sem=side_send, recv_sem=side_recv,
            device_id=near(*peer), device_id_type=MESH,
        ).start()
    for i, src in enumerate((weight, residual)):
        pltpu.make_async_copy(src, side_in.at[mine, i], side_recv).start()

    line = z * nc + c
    line_core = lax.rem(z, nc)
    takes_line = c == line_core
    owns_line = z == y * nc + c

    def line_target(dz):
        zo = lax.rem(z + dz, nz)
        return (y, zo, lax.rem(zo, nc), x)

    def line_column(dz):
        zo = lax.rem(z + dz, nz)
        return pl.multiple_of(((zo // nc * nz + zo) * nc + lax.rem(zo, nc)) * BLK, BLK)

    def send_side(dz):
        pltpu.make_async_remote_copy(
            src_ref=side_staged, dst_ref=line_side.at[line], send_sem=line_side_send, recv_sem=line_side_recv,
            device_id=line_target(dz), device_id_type=MESH,
        ).start()

    def send_line(dz):
        pltpu.make_async_remote_copy(
            src_ref=staged.at[:, pl.ds(line_column(dz), BLK)], dst_ref=line_words.at[line],
            send_sem=line_send, recv_sem=line_recv, device_id=line_target(dz), device_id_type=MESH,
        ).start()

    spread = sorted(range(1, nz), key=lambda d: -min(d, nz - d))
    for dz in spread:
        send_side(dz)

    @pl.when(takes_line)
    def _():
        for i, src in enumerate((weight, residual)):
            pltpu.make_async_copy(src, line_side.at[line, i], line_side_recv).start()
        pltpu.make_async_copy(genotypes.at[:, pl.ds(line_column(0), BLK)], line_words.at[line], line_recv).start()

    @pl.when(jnp.logical_not(takes_line))
    def _():
        send_side(0)

    stage.wait()
    for dz in spread:
        send_line(dz)
    pl.when(jnp.logical_not(takes_line))(lambda: send_line(0))

    def outward(core):
        middle = nz // 2
        return jnp.where(z < middle, 1, jnp.where(z > middle, -1, 1 - 2 * core))

    def owner_of(j, core):
        distance = nz // 2 - (j + 1) // 2
        sign = (2 * (j % 2) - 1) * outward(core)
        return lax.rem(z + sign * distance + nz, nz)

    def send_words(j, carry):
        def send(to):
            column = pl.multiple_of(((to[0] * nz + owner_of(j, to[2])) * nc + to[2]) * BLK, BLK)
            pltpu.make_async_remote_copy(
                src_ref=staged.at[:, pl.ds(column, BLK)], dst_ref=words.at[j, mine],
                send_sem=word_send, recv_sem=word_recv.at[j],
                device_id=to, device_id_type=MESH,
            ).start()

        for peer in near_peers:
            to = near(*peer)
            pl.when(owner_of(j, to[2]) != to[0] * nc + to[2])(functools.partial(send, to))

        @pl.when(owner_of(j, c) != mine)
        def _():
            column = pl.multiple_of(((y * nz + owner_of(j, c)) * nc + c) * BLK, BLK)
            pltpu.make_async_copy(
                genotypes.at[:, pl.ds(column, BLK)], words.at[j, mine], word_recv.at[j]
            ).start()

        return carry

    lax.fori_loop(0, nz, send_words, 0)

    lane = lax.broadcasted_iota(jnp.int32, (TAIL, BLK), 1)
    sublane = lax.broadcasted_iota(jnp.int32, (TAIL, BLK), 0)

    def prepare(side_ref, lhs_ref, scale_ref, tail_ref):
        count = side_ref.shape[0]
        width = count * rows
        weight_all, residual_all = (
            jnp.concatenate([side_ref[g, i] for g in range(count)], axis=1) for i in range(2)
        )
        rounded = weight_all.astype(BF16).astype(F32)
        cross = weight_all * residual_all
        high = cross.astype(BF16).astype(F32)
        low = (cross - high).astype(BF16).astype(F32)
        field = lax.broadcasted_iota(jnp.int32, (FIELDS, 1), 0)
        inverse = jnp.ones((FIELDS, 1), F32)
        for k in range(1, FIELDS):
            inverse = jnp.where(field == k, 0.25 ** min(k, FIELDS - 2), inverse)
        scale_ref[...] = rounded * (inverse * inverse)
        extra = [a * inverse for a in (rounded, high, low)]
        row_id = lax.broadcasted_iota(jnp.int32, (2 * TAIL, width), 0)
        for k in range(FIELDS):
            rows_k = jnp.zeros((2 * TAIL, width), F32)
            for i, a in enumerate(extra):
                rows_k = jnp.where(row_id == i, a[k : k + 1], rows_k)
            lhs_ref[BLK : BLK + 2 * TAIL, k * width : (k + 1) * width] = rows_k.astype(BF16)
        tail_rows = jnp.zeros((TAIL, BLK), F32)
        for i, s in enumerate((total(rounded), total(high + low), total(cross * residual_all))):
            tail_rows = jnp.where(sublane == 3 + i, s, tail_rows)
        tail_ref[...] = tail_rows

    pltpu.make_async_copy(side_in, side_in, side_recv).wait()
    prepare(side_in, lhs, scale, tail)

    @pl.when(takes_line)
    def _():
        pltpu.make_async_copy(line_side, line_side, line_side_recv).wait()
        prepare(line_side, line_lhs, line_scale, line_tail)

    fold_down = lax.broadcasted_iota(jnp.int32, (HALF, BLK), 0)
    fold_side = lax.broadcasted_iota(jnp.int32, (HALF, BLK), 1)
    folded = jnp.logical_and(fold_side >= HALF, fold_down >= fold_side - HALF)

    def reduce_block(block, lhs_ref, rhs_ref, scale_ref, tail_ref, to_ref):
        width = block.shape[0]
        turned = jnp.transpose(block)
        for k in range(FIELDS):
            at = slice(k * width, (k + 1) * width)
            rhs_ref[at, :] = masked(block, k).astype(BF16)
            lhs_ref[:BLK, at] = (masked(turned, k) * scale_ref[k : k + 1, :]).astype(BF16)
        gram = jnp.dot(lhs_ref[...], rhs_ref[...], preferred_element_type=F32)
        low_rows = gram[HALF:BLK]
        to_ref[:HALF] = jnp.where(folded, pltpu.roll(gram[:HALF], HALF, 1), low_rows)
        corner = jnp.sum(jnp.where(fold_side - HALF == fold_down, low_rows, 0.0), axis=0, keepdims=True)
        to_ref[HALF:] = gram[BLK : BLK + TAIL] + jnp.where(sublane == 6, corner, tail_ref[...])

    def partial(j):
        pltpu.make_async_copy(words.at[j], words.at[j], word_recv.at[j]).wait()
        reduce_block(words[j].reshape(depth, BLK), lhs, rhs, scale, tail, part.at[j])

    def far_block(j, carry):
        owner = owner_of(j, c)

        @pl.when(owner != mine)
        def _():
            partial(j)
            pltpu.make_async_remote_copy(
                src_ref=part.at[j], dst_ref=gathered.at[lax.rem(owner - z + nz, nz) - 1],
                send_sem=part_send, recv_sem=part_recv,
                device_id=(y, owner, c, x), device_id_type=MESH,
            ).start()

        return carry

    line_at = min(LINE_AT, nz - 1)
    lax.fori_loop(0, line_at, far_block, 0)

    @pl.when(takes_line)
    def _():
        pltpu.make_async_copy(line_words, line_words, line_recv).wait()
        block = line_words[...].reshape(nz * nc * rows, BLK)
        reduce_block(block, line_lhs, line_rhs, line_scale, line_tail, line_part)

        @pl.when(jnp.logical_not(owns_line))
        def _():
            pltpu.make_async_remote_copy(
                src_ref=line_part, dst_ref=line_in.at[y], send_sem=line_part_send, recv_sem=line_part_recv,
                device_id=(z // nc, z, c, x), device_id_type=MESH,
            ).start()

    lax.fori_loop(line_at, nz - 1, far_block, 0)
    pl.when(jnp.logical_not(owns_line))(lambda: partial(nz - 1))

    for copy in smalls:
        copy.wait()
    own = (y * nz + z) * nc + c
    doubled = 2.0 * freq_v[pl.ds(own, 1), :]
    own_block = x * (ny * nz * nc) + own
    bg = bg_v[...]
    block_id = lax.broadcasted_iota(jnp.int32, bg.shape, 0) * BLK + lax.broadcasted_iota(jnp.int32, bg.shape, 1)
    gene = total(jnp.where(block_id == own_block, bg, 0))
    first = total((bg < gene).astype(jnp.int32))
    row_lane = lax.broadcasted_iota(jnp.int32, (1, BLK), 1)
    counted = total(jnp.where(row_lane == gene, gv_v[...], 0))
    live = (own_block - first) * BLK + row_lane < counted
    effective = jnp.where(live, vw_v[pl.ds(own, 1), :], 0.0)

    @pl.when(owns_line)
    def _():
        span = line_in.at[pl.ds(0, ny - 1)]
        pltpu.make_async_copy(span, span, line_part_recv).wait()
        got = line_part[...]
        for dy in range(1, ny):
            got = got + line_in[lax.rem(y + dy, ny)]
        result[...] = got

    @pl.when(jnp.logical_not(owns_line))
    def _():
        pltpu.make_async_copy(gathered, gathered, part_recv).wait()
        got = part[nz - 1]
        for j in range(nz - 1):
            got = got + gathered[j]
        result[...] = got

    summed = result[...]
    ends = summed[HALF:]
    linear, weight_sum = ends[0:1], ends[3:4]
    score = ends[1:2] + ends[2:3] - doubled * ends[4:5]
    down = lax.broadcasted_iota(jnp.int32, (BLK, BLK), 0)
    stacked = jnp.where(down == 0, doubled, jnp.where(down == 1, linear, jnp.where(down == 2, effective, 0.0)))
    upright = jnp.transpose(stacked)

    def by_row(i):
        return jnp.where(folded, upright[:HALF, i : i + 1], upright[HALF:, i : i + 1])

    def by_lane(row):
        return jnp.where(folded, pltpu.roll(row, HALF, 1), row)

    doubled_v, linear_v = by_lane(doubled), by_lane(linear)
    gram = summed[:HALF] - by_row(0) * (linear_v - doubled_v * weight_sum) - by_row(1) * doubled_v
    scaled = by_row(2) * gram * by_lane(effective)
    first_diagonal = fold_side - HALF == fold_down
    twice = jnp.where(first_diagonal, 1.0, 2.0) * scaled
    corner = ends[6:7] - doubled * (2.0 * linear - doubled * weight_sum)
    corner = jnp.where(row_lane >= HALF, effective * effective * corner, 0.0)
    weighted_score = effective * score
    stats = (
        total(weighted_score),
        total(twice) + total(corner),
        total(weighted_score * weighted_score),
        total(jnp.where(first_diagonal, scaled, 0.0)) + total(corner),
        total(twice * scaled) + total(corner * corner),
    )
    near_gene = gene - (x * ny + y) * genes_here
    row = jnp.zeros((1, BLK), F32)
    for i, s in enumerate(stats):
        row = jnp.where(row_lane == i * genes_here + near_gene, s, row)
    at_variance = len(stats) * genes_here
    share = jnp.where(c == 0, tail[5:6, :], 0.0)
    row = jnp.where(row_lane == at_variance, share, row)
    seat = z * nc + c
    place = x * ny + y
    group = nz * nc
    places = nx * ny
    samples = depth * nz * FIELDS
    rows_one[seat] = row
    far_id = sum(i * (place == p).astype(jnp.int32) for i, p in enumerate(far_places))

    @pl.when(is_far)
    def _():
        pltpu.make_async_remote_copy(
            src_ref=rows_one.at[seat], dst_ref=rows_all.at[far_id * group + seat], send_sem=row_send, recv_sem=row_recv,
            device_id=(0, 0, head, 0), device_id_type=MESH,
        ).start()

    def send_row(dz):
        pltpu.make_async_remote_copy(
            src_ref=rows_one.at[seat], dst_ref=rows_one.at[seat], send_sem=one_send, recv_sem=one_recv,
            device_id=along(dz, head), device_id_type=MESH,
        ).start()

    for dz in range(1, nz):
        send_row(dz)

    @pl.when(c != head)
    def _():
        send_row(0)

    def added(rows_ref, base):
        genes = rows_ref[base]
        for i in range(1, group):
            genes = genes + rows_ref[base + i]
        return genes

    def scored(genes):
        lane_id = lax.broadcasted_iota(jnp.int32, genes.shape, 1)
        variance = jnp.sum(jnp.where(lane_id == at_variance, genes, 0.0), axis=1, keepdims=True) / samples
        totals = [genes] + [pltpu.roll(genes, BLK - i * genes_here, 1) for i in range(1, len(stats))]
        here = lane_id < genes_here
        totals = [jnp.where(here, t, 1.0) for t in totals]
        burden = totals[0] / jnp.sqrt(variance * totals[1])
        skat = (totals[2] - variance * totals[3]) / (variance * jnp.sqrt(2.0 * totals[4]))
        return [jnp.where(here, a, 0.0) for a in (burden, skat)]

    def merge(chosen):
        scores = rows_two[chosen[0]]
        for p in chosen[1:]:
            scores = scores + rows_two[p]
        return scores

    def finish():
        genes = jnp.concatenate([added(rows_all, i * group) for i in range(len(far_places))], axis=0)
        lane_id = lax.broadcasted_iota(jnp.int32, genes.shape, 1)
        row_id = lax.broadcasted_iota(jnp.int32, genes.shape, 0)
        place_id = sum(jnp.where(row_id == i, p, 0) for i, p in enumerate(far_places))
        near_scores = merge([p for p in range(places) if p not in far_places])
        for i, spread in enumerate(scored(genes)):
            width = genes_here
            while width < BLK:
                spread = spread + pltpu.roll(spread, width, 1)
                width *= 2
            spread = jnp.where(lane_id // genes_here == place_id, spread, 0.0)
            out[i : i + 1] = near_scores[i : i + 1] + jnp.sum(spread, axis=0, keepdims=True)

    def two_wait(count, sem):
        span = rows_two.at[pl.ds(0, count)]
        pltpu.make_async_copy(span, span, sem).wait()

    with_first = jnp.logical_and(z == 0, c == head)
    across_peers = [(dx, dy) for dx in range(nx) for dy in range(ny)]

    @pl.when(c == head)
    def _():
        span = rows_one.at[pl.ds(0, group - 1)]
        pltpu.make_async_copy(span, span, one_recv).wait()
        own_genes = added(rows_one, 0)
        pair_row = lax.broadcasted_iota(jnp.int32, (2, BLK), 0)
        burden, skat = (pltpu.roll(a, place * genes_here, 1) for a in scored(own_genes))
        rows_two[place] = jnp.where(pair_row == 0, burden, skat)

        def send_scores(to):
            pltpu.make_async_remote_copy(
                src_ref=rows_two.at[place], dst_ref=rows_two.at[place], send_sem=two_send, recv_sem=two_recv,
                device_id=to, device_id_type=MESH,
            ).start()

        for core in range(nc):
            for dx, dy in across_peers[::-1]:
                to = across(dx, dy, core)
                if core != head:
                    send_scores(to)
                elif dx + dy > 0:
                    pl.when(jnp.logical_not(with_first & is_far & (to[0] + to[3] == 0)))(
                        functools.partial(send_scores, to)
                    )

        @pl.when(is_first)
        def _():
            if places - 1 > len(far_places):
                two_wait(places - 1 - len(far_places), two_recv)
            span = rows_all.at[pl.ds(0, group * len(far_places))]
            pltpu.make_async_copy(span, span, row_recv).wait()
            finish()

        @pl.when(jnp.logical_not(is_first))
        def _():
            two_wait(places - 1, two_recv)
            out[...] = merge(range(places))

        skipped = with_first & is_far

        two_wait(places, two_send)
        pl.when(skipped)(lambda: two_wait(places - 2, two_send))
        pl.when(jnp.logical_not(skipped))(lambda: two_wait(places - 1, two_send))

    @pl.when(c != head)
    def _():
        two_wait(places, two_recv)
        out[...] = merge(range(places))
        pltpu.make_async_copy(rows_one.at[0], rows_one.at[0], one_send).wait()

    sent = len(near_peers)
    span = side_in.at[pl.ds(0, sent)]
    pltpu.make_async_copy(span, span, side_send).wait()
    span = words.at[pl.ds(0, nz - 1), pl.ds(0, sent)]
    pltpu.make_async_copy(span, span, word_send).wait()

    def sent_line(count):
        for ref, sem in ((line_side, line_side_send), (line_words, line_send)):
            span = ref.at[pl.ds(0, count)]
            pltpu.make_async_copy(span, span, sem).wait()

    pl.when(takes_line)(lambda: sent_line(nz - 1))
    pl.when(jnp.logical_not(takes_line))(lambda: sent_line(nz))

    @pl.when(jnp.logical_and(takes_line, jnp.logical_not(owns_line)))
    def _():
        pltpu.make_async_copy(line_part, line_part, line_part_send).wait()

    def sent_parts(count):
        span = gathered.at[pl.ds(0, count)]
        pltpu.make_async_copy(span, span, part_send).wait()

    pl.when(owns_line)(lambda: sent_parts(nz - 1))
    pl.when(jnp.logical_not(owns_line))(lambda: sent_parts(nz - 2))
    span = rows_one.at[pl.ds(0, nz - 1)]
    pltpu.make_async_copy(span, span, one_send).wait()

    @pl.when(is_far)
    def _():
        pltpu.make_async_copy(rows_all.at[0], rows_all.at[0], row_send).wait()


def local(
    sizes, genotypes, allele_freq, sample_weight, residual, variant_weight, block_gene, gene_variants
):
    ny, nz, nc, nx = sizes
    rows, columns = genotypes.shape
    group = ny * nc
    depth = group * rows
    blocks = columns // BLK
    args = (
        genotypes,
        allele_freq.reshape(blocks, BLK),
        sample_weight,
        residual,
        variant_weight.reshape(blocks, BLK),
        block_gene.reshape(-1, BLK),
        gene_variants.reshape(1, -1),
    )
    anywhere = pl.BlockSpec(memory_space=pl.ANY)
    dma = pltpu.SemaphoreType.DMA
    scores = pl.pallas_call(
        functools.partial(kernel, sizes),
        out_shape=pltpu.VMEM((2, BLK), F32),
        in_specs=[anywhere] * len(args),
        out_specs=pl.BlockSpec(memory_space=pltpu.VMEM),
        scratch_shapes=[
            pltpu.VMEM((rows, columns), jnp.int32),
            pltpu.VMEM((nz, group, rows, BLK), jnp.int32),
            pltpu.VMEM((2, FIELDS, rows), F32),
            pltpu.VMEM((group, 2, FIELDS, rows), F32),
            pltpu.VMEM((FIELDS * depth, BLK), BF16),
            pltpu.VMEM((BLK + 2 * TAIL, FIELDS * depth), BF16),
            pltpu.VMEM((FIELDS, depth), F32),
            pltpu.VMEM((TAIL, BLK), F32),
            pltpu.VMEM((nz, HALF + TAIL, BLK), F32),
            pltpu.VMEM((nz - 1, HALF + TAIL, BLK), F32),
            pltpu.VMEM(args[1].shape, F32),
            pltpu.VMEM(args[4].shape, F32),
            pltpu.VMEM(args[5].shape, jnp.int32),
            pltpu.VMEM(args[6].shape, jnp.int32),
            pltpu.VMEM((nz * nc, 1, BLK), F32),
            pltpu.VMEM((nx * ny, 2, BLK), F32),
            pltpu.VMEM((nx * ny * nz * nc, 1, BLK), F32),
            pltpu.VMEM((nz * nc, 2, FIELDS, rows), F32),
            pltpu.VMEM((nz * nc, rows, BLK), jnp.int32),
            pltpu.VMEM((FIELDS * nz * nc * rows, BLK), BF16),
            pltpu.VMEM((BLK + 2 * TAIL, FIELDS * nz * nc * rows), BF16),
            pltpu.VMEM((FIELDS, nz * nc * rows), F32),
            pltpu.VMEM((TAIL, BLK), F32),
            pltpu.VMEM((HALF + TAIL, BLK), F32),
            pltpu.VMEM((ny, HALF + TAIL, BLK), F32),
            pltpu.VMEM((HALF + TAIL, BLK), F32),
            dma, dma, dma, dma, dma, dma,
            dma, dma((2,)), dma((4,)), dma((nz,)), dma, dma, dma,
            dma, dma, dma, dma, dma, dma, dma, dma,
        ],
        compiler_params=pltpu.CompilerParams(collective_id=0, has_side_effects=True),
    )(*args)
    return (scores[0], scores[1])


def solution(mesh):
    nx = mesh.shape["gene"]
    sizes = (4, 8, 2, nx)
    torus = Mesh(mesh.devices.reshape(sizes), ("y", "z", "c", "x"))
    samp = ("y", "z", "c")
    placed = (P(samp, "x"), P("x"), P(None, samp), P(None, samp), P("x"), P(), P())
    step = functools.partial(local, sizes)
    return jax.shard_map(step, mesh=torus, in_specs=placed, out_specs=(P(), P()), check_vma=False)
```
